256 devices in a mesh: lev: 8 (over z), wav: 32 (over y, x, core).
Axes of the slice: x: 4, y: 4, z: 8, core: 2. Of those that a mesh axis runs over, the one named last changes fastest.
Arguments:
- grid_field: float32 [16, 1216, 1216], P('lev', 'wav'), may hold values from -6 to 6
- truncation_limit: int32 [1216], replicated, may hold values from -1 to 607, as said below
- diffusion_order: int32 [16], P('lev'), may hold values from 1 to 4
- diffusion_strength: float32 [16], P('lev'), may hold values from 2 to 50
- mass_weight: float32 [16], P('lev'), may hold values from 0.25 to 4
Outputs:
- filtered: float32 [16, 1216, 1216], P('lev', 'wav')
- energies: float32 [16], P('lev')
- total_energy: float32 [], replicated
The draws below stay inside these ranges and needn't reach their ends.
Inputs may be any that keep to these rules, and one draw needn't show every extreme that they name: `truncation_limit`: the largest |wavenumber(q)| kept at index p, with wavenumber(m) = m below 608 and m - 1216 otherwise; the kept set is an ellipse about wavenumber zero; the value at p equals the value at 1216 - p; -1 where nothing is kept; the value at p = 0 is 607.
All inputs are finite; a program needn't handle non-finite values.
Results may differ from the reference program's by a relative error of at most 0.000071.
Values sent between devices are 32-bit elements.
No kernel may reach another device: no remote copies, remote signals or barrier semaphores. Data moves between devices by JAX's collectives and lax.ppermute only.
A program may use at most 64 MiB of HBM per device.

```python
import math
import jax
import jax.numpy as jnp
from jax import lax

N = 1216
SLABS = 16


def draw_truncation_limit(key, part):
    axis_second = jax.random.randint(key, (), 3 * N // 10, N // 2)
    axis_first = N // 2 - 1
    positions = jnp.arange(N, dtype=jnp.int32)
    distance = jnp.abs(jnp.where(positions < N // 2, positions, positions - N))
    steps_first = jnp.arange(N // 2 + 1, dtype=jnp.int32)
    scaled_second = distance * 1000 // axis_second
    scaled_first = steps_first * 1000 // axis_first
    inside = scaled_second[:, None] ** 2 + scaled_first[None, :] ** 2 <= 1000000
    return (jnp.sum(inside.astype(jnp.int32), axis=1) - 1).astype(jnp.int32)


def set_ends(drawn, key, smallest, largest):
    place = [jax.random.randint(jax.random.fold_in(key, axis), (), 0, length) for axis, length in enumerate(drawn.shape)]
    longest = drawn.shape.index(max(drawn.shape))
    neighbour = place[:longest] + [(place[longest] + 1) % drawn.shape[longest]] + place[longest + 1:]
    return drawn.at[tuple(place)].set(smallest).at[tuple(neighbour)].set(largest)


def block_levels(key, extent, pieces, low, largest):
    loudness, own = 1.0, jax.random.fold_in(key, 6)
    for position, shards_of in pieces:
        draws = jnp.exp(jax.random.uniform(jax.random.fold_in(own, position), (shards_of,), jnp.float32, low / len(pieces), largest / len(pieces)))
        loudness = loudness * jnp.repeat(draws, extent[position] // shards_of).reshape([-1 if axis == position else 1 for axis in range(len(extent))])
    return loudness


def centred(own_key, extent, spread, bound, split=(), kind=jnp.bfloat16):
    gain = block_levels(own_key, extent, split, -0.22, 0.18) if split else 1.0
    drawn = jax.random.normal(own_key, extent, jnp.float32) * spread * gain
    return jnp.minimum(jnp.maximum(drawn, -bound), bound).astype(kind)


def setup_inputs(seed: int = 0) -> dict:
    key_list = jax.random.split(jax.random.key(seed), 6)
    grid_field = centred(key_list[0], (SLABS, N, N), 1.0, 6.0, ((0, 8), (1, 32)), jnp.float32)
    truncation_limit = draw_truncation_limit(jax.random.fold_in(key_list[5], 71), 0)
    diffusion_order = set_ends(jax.random.randint(key_list[2], (SLABS,), 1, 5), jax.random.fold_in(key_list[2], 1), 1, 4).astype(jnp.int32)
    diffusion_strength = jnp.clip(jnp.exp(math.log(50.0) - 3.218876 * jax.random.uniform(key_list[3], (SLABS,), jnp.float32) ** block_levels(key_list[3], (SLABS,), ((0, 8),), -0.2, 0.2)), 2.0, 50.0)
    mass_weight = jnp.clip(jnp.exp(math.log(4.0) - 2.7725887 * jax.random.uniform(key_list[4], (SLABS,), jnp.float32) ** block_levels(key_list[4], (SLABS,), ((0, 8),), -0.2, 0.2)), 0.25, 4.0)
    return dict(grid_field=grid_field, truncation_limit=truncation_limit, diffusion_order=diffusion_order, diffusion_strength=diffusion_strength, mass_weight=mass_weight)


def signed(positions, length):
    return jnp.where(positions < length // 2, positions, positions - length)


def reference(grid_field, truncation_limit, diffusion_order, diffusion_strength, mass_weight):
    positions = jnp.arange(N, dtype=jnp.int32)
    signed_index = signed(positions, N)
    wavenumber = signed_index.astype(jnp.float32)
    scaled_radius = (wavenumber[:, None] ** 2 + wavenumber[None, :] ** 2) / (0.5 * N) ** 2
    inside = (jnp.abs(signed_index)[None, :] <= truncation_limit[:, None]).astype(jnp.float32)

    def one_slab(members):
        slab_field, degree, strength = members
        spectrum = jnp.fft.fft2(slab_field).T
        damping = inside / (1.0 + strength * jnp.power(scaled_radius, degree.astype(jnp.float32)))
        damped = spectrum * damping
        energy = jnp.sum(jnp.real(damped) ** 2 + jnp.imag(damped) ** 2) / float(N) ** 4
        filtered = jnp.real(jnp.fft.ifft2(damped.T))
        return filtered, energy

    filtered, energies = lax.map(one_slab, (grid_field, diffusion_order, diffusion_strength))
    total_energy = jnp.sum(mass_weight * energies) / SLABS
    return filtered, energies, total_energy
```

```python
import functools
import math

import jax
import jax.numpy as jnp
import ml_dtypes
import numpy as np
from jax import lax
from jax.experimental import pallas as pl
from jax.experimental.pallas import tpu as pltpu
from jax.sharding import PartitionSpec as P

N = 1216
HALF = N // 2
PEERS = 32
ROWS = N // PEERS
PITCH = 40
WAVES = HALF // PEERS
SIDE = PEERS // 2
BLOCK = SIDE * PITCH
PAIR = 2 * PITCH


def split(table):
    high = table.astype(ml_dtypes.bfloat16)
    low = (table - high.astype(np.float64)).astype(ml_dtypes.bfloat16)
    return high, low


def angle(product):
    return (product % N).astype(np.float64) * (2.0 * math.pi / N)


def lane_waves():
    waves = np.full((2, SIDE, 32), -1, np.int64)
    for parity in range(2):
        for place in range(SIDE):
            waves[parity, place, :WAVES] = 2 * (place * WAVES + np.arange(WAVES)) + parity
    waves[0, 0, WAVES] = HALF
    return waves


@functools.cache
def row_tables():
    waves = lane_waves()
    j = np.arange(HALF)
    forward, back = [], []
    for parity in range(2):
        wave = waves[parity]
        used = (wave >= 0).astype(np.float64)
        theta = angle(j[:, None, None] * np.maximum(wave, 0))
        cosine, sine = np.cos(theta) * used, np.sin(theta) * used
        sine = np.where(wave % HALF == 0, 0.0, sine)
        forward.append(np.stack([cosine, -sine], axis=2).reshape(HALF, SIDE * 64))
        weight = np.where(wave % HALF == 0, 1.0, 2.0) / float(N) ** 2
        back.append(
            np.stack([cosine * weight, -sine * weight], axis=2).reshape(HALF, SIDE * 64).T
        )
    return (
        np.stack([np.stack(split(t)) for t in forward]),
        np.stack([np.stack(split(np.ascontiguousarray(t))) for t in back]),
    )


@functools.cache
def column_tables():
    place = np.full((SIDE, PITCH), -1, np.int64)
    place[:, :ROWS] = np.arange(HALF).reshape(SIDE, ROWS)
    place = place.reshape(-1)
    used = (place >= 0).astype(np.float64)
    spot = np.maximum(place, 0)
    m = np.arange(HALF)
    forward, back = [], []
    for parity in range(2):
        theta = angle((2 * m + parity)[:, None] * spot[None, :])
        cosine, sine = np.cos(theta) * used, np.sin(theta) * used
        forward.append(np.concatenate(split(np.concatenate([cosine, sine], axis=1)), axis=0))
        back.append(np.concatenate(split(np.concatenate([cosine.T, -sine.T], axis=1)), axis=0))
    return np.stack(forward), np.stack(back)


def dot(left, right):
    return lax.dot_general(left, right, (((1,), (0,)), ((), ())), preferred_element_type=jnp.float32)


def halves(values):
    high = values.astype(jnp.bfloat16)
    low = (values - high.astype(jnp.float32)).astype(jnp.bfloat16)
    return high, low


def lane_index(rows):
    return lax.broadcasted_iota(jnp.int32, (rows, 128), 1)


def row_kernel(x_ref, table_ref, out_ref, xs, held, sem):
    chunk = 512
    copies = []
    for parity in range(2):
        for k in range(2):
            for part in range(2):
                slot = (parity * 2 + k) * 2 + part
                copy = pltpu.make_async_copy(
                    table_ref.at[parity, part, :, pl.ds(k * chunk, chunk)],
                    held.at[parity, part, :, pl.ds(k * chunk, chunk)],
                    sem.at[slot],
                )
                copy.start()
                copies.append(copy)
    xs[...] = jnp.zeros_like(xs)
    for slab in range(2):
        xs[slab * PITCH : slab * PITCH + ROWS, :N] = x_ref[slab]
    full = xs[...]
    turned = pltpu.roll(full, full.shape[1] - HALF, 1)
    left_lanes = lane_index(PITCH) < 64
    for parity in range(2):
        value = (full + turned if parity == 0 else full - turned)[:, :HALF]
        high, low = halves(value)
        both = jnp.concatenate([high, low], axis=0)
        for k in range(2):
            for part in range(2):
                copies[(parity * 2 + k) * 2 + part].wait()
            columns = slice(k * chunk, (k + 1) * chunk)
            main = dot(both, held[parity, 0, :, columns])
            result = main[:PAIR] + main[PAIR:] + dot(high, held[parity, 1, :, columns])
            for v in range(chunk // 128):
                first = result[:PITCH, v * 128 : (v + 1) * 128]
                second = result[PITCH:, v * 128 : (v + 1) * 128]
                peer = parity * SIDE + k * (chunk // 64) + 2 * v
                out_ref[peer] = jnp.where(left_lanes, first, pltpu.roll(second, 64, 1))
                out_ref[peer + 1] = jnp.where(left_lanes, pltpu.roll(first, 64, 1), second)


def damp_kernel(lane_ref, out_ref):
    wave_square = lane_ref[0:1, :]
    limit = lane_ref[1:2, :]
    order = lane_ref[2:3, :]
    strength = lane_ref[3:4, :]
    for parity in range(2):
        m = lax.broadcasted_iota(jnp.int32, (HALF, 128), 0)
        q = 2 * m + parity
        wave = jnp.where(q < HALF, q, q - N).astype(jnp.float32)
        radius = (wave_square + wave * wave) / (0.5 * N) ** 2
        square = radius * radius
        powered = jnp.where(
            order == 1.0,
            radius,
            jnp.where(order == 2.0, square, jnp.where(order == 3.0, square * radius, square * square)),
        )
        inside = (jnp.abs(wave) <= limit).astype(jnp.float32)
        out_ref[parity] = inside / (1.0 + strength * powered)


def swapped(values):
    real_lanes = (lane_index(values.shape[0]) // 32) % 2 == 0
    return jnp.where(real_lanes, pltpu.roll(values, 96, 1), -pltpu.roll(values, 32, 1))


def weights(values):
    other = swapped(values)
    return jnp.concatenate(
        [
            jnp.concatenate(halves(values), axis=1),
            jnp.concatenate(halves(other), axis=1),
        ],
        axis=0,
    )


def folded(result):
    count = result.shape[0] // 2
    total = result[:count] + result[count:]
    return total[:, :128] + total[:, 128:]


def column_kernel(in_ref, damp_ref, lane_ref, forward_ref, back_ref, out_ref):
    lower = in_ref[:SIDE].reshape(BLOCK, 128)
    upper = in_ref[SIDE:].reshape(BLOCK, 128)
    energy = jnp.zeros((1, 128), jnp.float32)
    parts = []
    for parity in range(2):
        value = lower + upper if parity == 0 else lower - upper
        spectrum = folded(dot(forward_ref[parity], weights(value)))
        damped = spectrum * damp_ref[parity]
        energy = energy + jnp.sum(damped * damped, axis=0, keepdims=True)
        parts.append(folded(dot(back_ref[parity], weights(damped))))
    out_ref[:SIDE] = (parts[0] + parts[1]).reshape(SIDE, PITCH, 128)
    out_ref[SIDE:] = (parts[0] - parts[1]).reshape(SIDE, PITCH, 128)
    energy = energy * lane_ref[4:5, :]
    for peer in range(PEERS):
        out_ref[peer, ROWS : ROWS + 1, :] = energy


def back_kernel(in_ref, table_ref, out_ref):
    left_lanes = lane_index(PITCH) < 64
    parts = []
    for parity in range(2):
        first, second = [], []
        for v in range(SIDE // 2):
            one = in_ref[parity * SIDE + 2 * v]
            two = in_ref[parity * SIDE + 2 * v + 1]
            first.append(jnp.where(left_lanes, one, pltpu.roll(two, 64, 1)))
            second.append(jnp.where(left_lanes, pltpu.roll(one, 64, 1), two))
        value = jnp.concatenate(
            [jnp.concatenate(first, axis=1), jnp.concatenate(second, axis=1)], axis=0
        )
        high, low = halves(value)
        main = dot(jnp.concatenate([high, low], axis=0), table_ref[parity, 0])
        parts.append(main[:PAIR] + main[PAIR:] + dot(high, table_ref[parity, 1]))
    lower, upper = parts[0] + parts[1], parts[0] - parts[1]
    for slab in range(2):
        rows = slice(slab * PITCH, slab * PITCH + ROWS)
        out_ref[slab, :, :HALF] = lower[rows]
        out_ref[slab, :, HALF:] = upper[rows]


VMEM = pl.BlockSpec(memory_space=pltpu.VMEM)
ANY = pl.BlockSpec(memory_space=pl.ANY)


def local(grid_field, truncation_limit, diffusion_order, diffusion_strength, mass_weight):
    row_forward, row_back = row_tables()
    column_forward, column_back = column_tables()
    block = jax.ShapeDtypeStruct((PEERS, PITCH, 128), jnp.float32)
    sent = pl.pallas_call(
        row_kernel,
        out_shape=block,
        in_specs=[VMEM, ANY],
        out_specs=VMEM,
        scratch_shapes=[
            pltpu.VMEM((PAIR, 1280), jnp.float32),
            pltpu.VMEM((2, 2, HALF, SIDE * 64), jnp.bfloat16),
            pltpu.SemaphoreType.DMA((8,)),
        ],
        name="row_forward",
    )(grid_field, jnp.asarray(row_forward))
    received = lax.all_to_all(sent, "wav", split_axis=0, concat_axis=0, tiled=True)

    place = lax.axis_index("wav")
    parity, spot = place // SIDE, place % SIDE
    chosen = jnp.where(parity == 0, truncation_limit[0:HALF:2], truncation_limit[1:HALF:2])
    limits = lax.dynamic_slice(chosen, (spot * WAVES,), (WAVES,))
    slots = jnp.arange(32, dtype=jnp.int32)
    limits = jnp.concatenate(
        [limits, truncation_limit[HALF : HALF + 1], jnp.full((32 - WAVES - 1,), -1, jnp.int32)]
    )
    wave = jnp.where(slots < WAVES, 2 * (spot * WAVES + slots) + parity, HALF)
    used = (slots < WAVES) | ((slots == WAVES) & (place == 0))
    weight = jnp.where(wave % HALF == 0, 1.0, 2.0) / float(N) ** 4
    weight = jnp.where(used, weight, 0.0)
    wave = wave.astype(jnp.float32)
    per_slab = lambda v: jnp.repeat(v.astype(jnp.float32), 64)
    lanes = jnp.stack(
        [
            jnp.tile(wave * wave, 4),
            jnp.tile(limits.astype(jnp.float32), 4),
            per_slab(diffusion_order),
            per_slab(diffusion_strength),
            jnp.tile(weight, 4),
        ]
        + [jnp.zeros((128,), jnp.float32)] * 3
    )
    damp = pl.pallas_call(
        damp_kernel,
        out_shape=jax.ShapeDtypeStruct((2, HALF, 128), jnp.float32),
        in_specs=[VMEM],
        out_specs=VMEM,
        cost_estimate=pl.CostEstimate(flops=20_000_000, bytes_accessed=600_000, transcendentals=0),
        name="damping",
    )(lanes)
    back = pl.pallas_call(
        column_kernel,
        out_shape=block,
        in_specs=[VMEM] * 5,
        out_specs=VMEM,
        name="column",
    )(received, damp, lanes, jnp.asarray(column_forward), jnp.asarray(column_back))
    returned = lax.all_to_all(back, "wav", split_axis=0, concat_axis=0, tiled=True)
    energies = jnp.sum(jnp.sum(returned[:, ROWS, :], axis=0).reshape(2, 64), axis=1)
    weighted = jnp.sum(mass_weight * energies)
    levels = lax.axis_size("lev")
    everyone = lax.all_to_all(
        jnp.broadcast_to(weighted, (levels, 128)), "lev", split_axis=0, concat_axis=0, tiled=True
    )
    total_energy = jnp.sum(everyone[:, 0]) / (2 * levels)
    filtered = pl.pallas_call(
        back_kernel,
        out_shape=jax.ShapeDtypeStruct(grid_field.shape, jnp.float32),
        in_specs=[VMEM] * 2,
        out_specs=VMEM,
        cost_estimate=pl.CostEstimate(flops=2_000_000_000, bytes_accessed=6_000_000, transcendentals=0),
        name="row_back",
    )(returned, jnp.asarray(row_back))
    return filtered, energies, total_energy


def solution(mesh):
    placed = (P("lev", "wav", None), P(), P("lev"), P("lev"), P("lev"))
    return jax.shard_map(
        local,
        mesh=mesh,
        in_specs=placed,
        out_specs=(P("lev", "wav", None), P("lev"), P()),
        check_vma=False,
    )
```

```python
import functools
import math

import jax
import jax.numpy as jnp
import ml_dtypes
import numpy as np
from jax import lax
from jax.experimental import pallas as pl
from jax.experimental.pallas import tpu as pltpu
from jax.sharding import PartitionSpec as P

N = 1216
HALF = N // 2
PEERS = 32
ROWS = N // PEERS
PITCH = 40
WAVES = HALF // PEERS
SIDE = PEERS // 2
BLOCK = SIDE * PITCH
PAIR = 2 * PITCH


def split(table):
    high = table.astype(ml_dtypes.bfloat16)
    low = (table - high.astype(np.float64)).astype(ml_dtypes.bfloat16)
    return high, low


def angle(product):
    return (product % N).astype(np.float64) * (2.0 * math.pi / N)


def lane_waves():
    waves = np.full((2, SIDE, 32), -1, np.int64)
    for parity in range(2):
        for place in range(SIDE):
            waves[parity, place, :WAVES] = 2 * (place * WAVES + np.arange(WAVES)) + parity
    waves[0, 0, WAVES] = HALF
    return waves


@functools.cache
def row_tables():
    waves = lane_waves()
    j = np.arange(HALF)
    forward, back = [], []
    for parity in range(2):
        wave = waves[parity]
        used = (wave >= 0).astype(np.float64)
        theta = angle(j[:, None, None] * np.maximum(wave, 0))
        cosine, sine = np.cos(theta) * used, np.sin(theta) * used
        sine = np.where(wave % HALF == 0, 0.0, sine)
        forward.append(np.stack([cosine, -sine], axis=2).reshape(HALF, SIDE * 64))
        weight = np.where(wave % HALF == 0, 1.0, 2.0) / float(N) ** 2
        back.append(
            np.stack([cosine * weight, -sine * weight], axis=2).reshape(HALF, SIDE * 64).T
        )
    return (
        np.stack([np.stack(split(t)) for t in forward]),
        np.stack([np.stack(split(np.ascontiguousarray(t))) for t in back]),
    )


@functools.cache
def column_tables():
    place = np.full((SIDE, PITCH), -1, np.int64)
    place[:, :ROWS] = np.arange(HALF).reshape(SIDE, ROWS)
    place = place.reshape(-1)
    used = (place >= 0).astype(np.float64)
    spot = np.maximum(place, 0)
    m = np.arange(HALF)
    forward, back = [], []
    for parity in range(2):
        theta = angle((2 * m + parity)[:, None] * spot[None, :])
        cosine, sine = np.cos(theta) * used, np.sin(theta) * used
        forward.append(np.concatenate(split(np.concatenate([cosine, sine], axis=1)), axis=0))
        back.append(np.concatenate(split(np.concatenate([cosine.T, -sine.T], axis=1)), axis=0))
    return np.stack(forward), np.stack(back)


def dot(left, right):
    return lax.dot_general(left, right, (((1,), (0,)), ((), ())), preferred_element_type=jnp.float32)


def halves(values):
    high = values.astype(jnp.bfloat16)
    low = (values - high.astype(jnp.float32)).astype(jnp.bfloat16)
    return high, low


def lane_index(rows):
    return lax.broadcasted_iota(jnp.int32, (rows, 128), 1)


def row_kernel(x_ref, table_ref, out_ref, xs, held, sem):
    chunk = 512
    copies = []
    for parity in range(2):
        for k in range(2):
            for part in range(2):
                slot = (parity * 2 + k) * 2 + part
                copy = pltpu.make_async_copy(
                    table_ref.at[parity, part, :, pl.ds(k * chunk, chunk)],
                    held.at[parity, part, :, pl.ds(k * chunk, chunk)],
                    sem.at[slot],
                )
                copy.start()
                copies.append(copy)
    xs[...] = jnp.zeros_like(xs)
    for slab in range(2):
        xs[slab * PITCH : slab * PITCH + ROWS, :N] = x_ref[:, slab, :]
    full = xs[...]
    turned = pltpu.roll(full, full.shape[1] - HALF, 1)
    left_lanes = lane_index(PITCH) < 64
    for parity in range(2):
        value = (full + turned if parity == 0 else full - turned)[:, :HALF]
        high, low = halves(value)
        both = jnp.concatenate([high, low], axis=0)
        for k in range(2):
            for part in range(2):
                copies[(parity * 2 + k) * 2 + part].wait()
            columns = slice(k * chunk, (k + 1) * chunk)
            main = dot(both, held[parity, 0, :, columns])
            result = main[:PAIR] + main[PAIR:] + dot(high, held[parity, 1, :, columns])
            for v in range(chunk // 128):
                first = result[:PITCH, v * 128 : (v + 1) * 128]
                second = result[PITCH:, v * 128 : (v + 1) * 128]
                peer = parity * SIDE + k * (chunk // 64) + 2 * v
                out_ref[peer] = jnp.where(left_lanes, first, pltpu.roll(second, 64, 1))
                out_ref[peer + 1] = jnp.where(left_lanes, pltpu.roll(first, 64, 1), second)


def damp_kernel(lane_ref, out_ref):
    wave_square = lane_ref[0:1, :]
    limit = lane_ref[1:2, :]
    order = lane_ref[2:3, :]
    strength = lane_ref[3:4, :]
    for parity in range(2):
        m = lax.broadcasted_iota(jnp.int32, (HALF, 128), 0)
        q = 2 * m + parity
        wave = jnp.where(q < HALF, q, q - N).astype(jnp.float32)
        radius = (wave_square + wave * wave) / (0.5 * N) ** 2
        square = radius * radius
        powered = jnp.where(
            order == 1.0,
            radius,
            jnp.where(order == 2.0, square, jnp.where(order == 3.0, square * radius, square * square)),
        )
        inside = (jnp.abs(wave) <= limit).astype(jnp.float32)
        out_ref[parity] = inside / (1.0 + strength * powered)


def swapped(values):
    real_lanes = (lane_index(values.shape[0]) // 32) % 2 == 0
    return jnp.where(real_lanes, pltpu.roll(values, 96, 1), -pltpu.roll(values, 32, 1))


def weights(values):
    other = swapped(values)
    return jnp.concatenate(
        [
            jnp.concatenate(halves(values), axis=1),
            jnp.concatenate(halves(other), axis=1),
        ],
        axis=0,
    )


def folded(result):
    count = result.shape[0] // 2
    total = result[:count] + result[count:]
    return total[:, :128] + total[:, 128:]


def column_kernel(in_ref, damp_ref, lane_ref, forward_ref, back_ref, out_ref):
    lower = in_ref[:SIDE].reshape(BLOCK, 128)
    upper = in_ref[SIDE:].reshape(BLOCK, 128)
    energy = jnp.zeros((1, 128), jnp.float32)
    parts = []
    for parity in range(2):
        value = lower + upper if parity == 0 else lower - upper
        spectrum = folded(dot(forward_ref[parity], weights(value)))
        damped = spectrum * damp_ref[parity]
        energy = energy + jnp.sum(damped * damped, axis=0, keepdims=True)
        parts.append(folded(dot(back_ref[parity], weights(damped))))
    out_ref[:SIDE] = (parts[0] + parts[1]).reshape(SIDE, PITCH, 128)
    out_ref[SIDE:] = (parts[0] - parts[1]).reshape(SIDE, PITCH, 128)
    energy = energy * lane_ref[4:5, :]
    for peer in range(PEERS):
        out_ref[peer, ROWS : ROWS + 1, :] = energy


def back_kernel(in_ref, table_ref, out_ref):
    left_lanes = lane_index(PITCH) < 64
    parts = []
    for parity in range(2):
        first, second = [], []
        for v in range(SIDE // 2):
            one = in_ref[parity * SIDE + 2 * v]
            two = in_ref[parity * SIDE + 2 * v + 1]
            first.append(jnp.where(left_lanes, one, pltpu.roll(two, 64, 1)))
            second.append(jnp.where(left_lanes, pltpu.roll(one, 64, 1), two))
        value = jnp.concatenate(
            [jnp.concatenate(first, axis=1), jnp.concatenate(second, axis=1)], axis=0
        )
        high, low = halves(value)
        main = dot(jnp.concatenate([high, low], axis=0), table_ref[parity, 0])
        parts.append(main[:PAIR] + main[PAIR:] + dot(high, table_ref[parity, 1]))
    lower, upper = parts[0] + parts[1], parts[0] - parts[1]
    for slab in range(2):
        rows = slice(slab * PITCH, slab * PITCH + ROWS)
        out_ref[:, slab, :HALF] = lower[rows]
        out_ref[:, slab, HALF:] = upper[rows]


def grant(mebibytes):
    return pltpu.CompilerParams(vmem_limit_bytes=mebibytes << 20)


VMEM = pl.BlockSpec(memory_space=pltpu.VMEM)
ANY = pl.BlockSpec(memory_space=pl.ANY)


def local(grid_field, truncation_limit, diffusion_order, diffusion_strength, mass_weight):
    row_forward, row_back = row_tables()
    column_forward, column_back = column_tables()
    block = jax.ShapeDtypeStruct((PEERS, PITCH, 128), jnp.float32)
    sent = pl.pallas_call(
        row_kernel,
        out_shape=block,
        in_specs=[VMEM, ANY],
        out_specs=VMEM,
        scratch_shapes=[
            pltpu.VMEM((PAIR, 1280), jnp.float32),
            pltpu.VMEM((2, 2, HALF, SIDE * 64), jnp.bfloat16),
            pltpu.SemaphoreType.DMA((8,)),
        ],
        compiler_params=grant(14),
        name="row_forward",
    )(grid_field.transpose(1, 0, 2), jnp.asarray(row_forward))
    received = lax.all_to_all(sent, "wav", split_axis=0, concat_axis=0, tiled=True)

    place = lax.axis_index("wav")
    parity, spot = place // SIDE, place % SIDE
    chosen = jnp.where(parity == 0, truncation_limit[0:HALF:2], truncation_limit[1:HALF:2])
    limits = lax.dynamic_slice(chosen, (spot * WAVES,), (WAVES,))
    slots = jnp.arange(32, dtype=jnp.int32)
    limits = jnp.concatenate(
        [limits, truncation_limit[HALF : HALF + 1], jnp.full((32 - WAVES - 1,), -1, jnp.int32)]
    )
    wave = jnp.where(slots < WAVES, 2 * (spot * WAVES + slots) + parity, HALF)
    used = (slots < WAVES) | ((slots == WAVES) & (place == 0))
    weight = jnp.where(wave % HALF == 0, 1.0, 2.0) / float(N) ** 4
    weight = jnp.where(used, weight, 0.0)
    wave = wave.astype(jnp.float32)
    per_slab = lambda v: jnp.repeat(v.astype(jnp.float32), 64)
    lanes = jnp.stack(
        [
            jnp.tile(wave * wave, 4),
            jnp.tile(limits.astype(jnp.float32), 4),
            per_slab(diffusion_order),
            per_slab(diffusion_strength),
            jnp.tile(weight, 4),
        ]
        + [jnp.zeros((128,), jnp.float32)] * 3
    )
    damp = pl.pallas_call(
        damp_kernel,
        out_shape=jax.ShapeDtypeStruct((2, HALF, 128), jnp.float32),
        in_specs=[VMEM],
        out_specs=VMEM,
        cost_estimate=pl.CostEstimate(flops=20_000_000, bytes_accessed=600_000, transcendentals=0),
        compiler_params=grant(4),
        name="damping",
    )(lanes)
    back = pl.pallas_call(
        column_kernel,
        out_shape=block,
        in_specs=[VMEM] * 5,
        out_specs=VMEM,
        compiler_params=grant(14),
        name="column",
    )(received, damp, lanes, jnp.asarray(column_forward), jnp.asarray(column_back))
    returned = lax.all_to_all(back, "wav", split_axis=0, concat_axis=0, tiled=True)
    energies = jnp.sum(jnp.sum(returned[:, ROWS, :], axis=0).reshape(2, 64), axis=1)
    weighted = jnp.sum(mass_weight * energies)
    levels = lax.axis_size("lev")
    everyone = lax.all_to_all(
        jnp.broadcast_to(weighted, (levels, 128)), "lev", split_axis=0, concat_axis=0, tiled=True
    )
    total_energy = jnp.sum(everyone[:, 0]) / (2 * levels)
    filtered = pl.pallas_call(
        back_kernel,
        out_shape=jax.ShapeDtypeStruct((ROWS, 2, N), jnp.float32),
        in_specs=[VMEM] * 2,
        out_specs=VMEM,
        cost_estimate=pl.CostEstimate(flops=2_000_000_000, bytes_accessed=6_000_000, transcendentals=0),
        compiler_params=grant(10),
        name="row_back",
    )(returned, jnp.asarray(row_back))
    return filtered.transpose(1, 0, 2), energies, total_energy


def solution(mesh):
    placed = (P("lev", "wav", None), P(), P("lev"), P("lev"), P("lev"))
    return jax.shard_map(
        local,
        mesh=mesh,
        in_specs=placed,
        out_specs=(P("lev", "wav", None), P("lev"), P()),
        check_vma=False,
    )
```

```python
import functools
import math

import jax
import jax.numpy as jnp
import ml_dtypes
import numpy as np
from jax import lax
from jax.experimental import pallas as pl
from jax.experimental.pallas import tpu as pltpu
from jax.sharding import PartitionSpec as P

N = 1216
HALF = N // 2
QUARTER = N // 4
PEERS = 32
ROWS = N // PEERS
PITCH = 40
WAVES = HALF // PEERS
WIDTH = 2 * WAVES
SIDE = PEERS // 2
GROUP = 3
COLUMNS = -(-SIDE // GROUP) * 128
PAIR = 2 * PITCH
SLOTS = {
    (0, 0): [(0, 0, 0, WIDTH)],
    (0, 1): [(1, 0, 0, WIDTH)],
    (0, 2): [(2, 0, 0, WIDTH)],
    (1, 0): [(0, 38, 0, WIDTH)],
    (1, 1): [(1, 38, 0, WIDTH)],
    (1, 2): [(2, 38, 0, WIDTH)],
    (0, 3): [(0, 76, 0, WIDTH)],
    (1, 3): [(1, 76, 0, WIDTH)],
    (0, 4): [(2, 76, 0, WIDTH)],
    (1, 4): [(0, 114, 0, 14), (1, 114, 14, 14), (2, 114, 28, 10)],
}


def split(table):
    high = table.astype(ml_dtypes.bfloat16)
    low = (table - high.astype(np.float64)).astype(ml_dtypes.bfloat16)
    return high, low


def angle(product):
    return (product % N).astype(np.float64) * (2.0 * math.pi / N)


@functools.cache
def row_tables():
    j = np.arange(HALF)
    forward = np.zeros((2, HALF, COLUMNS))
    back = np.zeros((2, COLUMNS, HALF))
    for parity in range(2):
        for place in range(SIDE):
            wave = 2 * (place * WAVES + np.arange(WAVES)) + parity
            theta = angle(j[:, None] * wave[None, :])
            cosine, sine = np.cos(theta), -np.sin(theta)
            weight = np.where(wave == 0, 1.0, 2.0)
            if wave[0] == 0:
                sine[:, 0] = np.cos(angle(j * HALF))
            both = np.concatenate([cosine, sine], axis=1)
            start = place // GROUP * 128 + place % GROUP * WIDTH
            forward[parity, :, start : start + WIDTH] = both
            back[parity, start : start + WIDTH, :] = (
                both * np.concatenate([weight, weight]) / float(N) ** 2
            ).T
    return (
        np.stack([np.stack(split(t)) for t in forward]),
        np.stack([np.stack(split(t)) for t in back]),
    )


@functools.cache
def column_tables():
    place = np.full((PEERS // 4, PITCH), -1, np.int64)
    place[:, :ROWS] = np.arange(QUARTER).reshape(PEERS // 4, ROWS)
    place = place.reshape(-1)
    used = (place >= 0).astype(np.float64)
    spot = np.maximum(place, 0)
    m = np.arange(QUARTER)
    forward, back = [], []
    for residue in range(4):
        theta = angle((4 * m + residue)[:, None] * spot[None, :])
        cosine, sine = np.cos(theta) * used, np.sin(theta) * used
        forward.append(np.concatenate(split(np.concatenate([cosine, sine], axis=1)), axis=0))
        back.append(np.concatenate(split(np.concatenate([cosine.T, -sine.T], axis=1)), axis=0))
    return np.stack(forward), np.stack(back)


def dot(left, right):
    return lax.dot_general(left, right, (((1,), (0,)), ((), ())), preferred_element_type=jnp.float32)


def halves(values):
    high = values.astype(jnp.bfloat16)
    low = (values - high.astype(jnp.float32)).astype(jnp.bfloat16)
    return high, low


def lane_index(rows):
    return lax.broadcasted_iota(jnp.int32, (rows, 128), 1)


def turn(values, shift):
    return values if shift % 128 == 0 else pltpu.roll(values, shift % 128, 1)


def gather_lanes(pieces):
    lane = lane_index(8)
    result = None
    for values, source, target in pieces:
        turned = turn(values, target - source)
        result = turned if result is None else jnp.where(lane >= target, turned, result)
    return result


def packed(read):
    tiles = []
    for tile in range(3):
        pieces = []
        for (slab, r), slots in SLOTS.items():
            for where, lane, first, _ in slots:
                if where == tile:
                    values, start = read(slab, r)
                    pieces.append((values, start + first, lane))
        tiles.append(gather_lanes(sorted(pieces, key=lambda p: p[2])))
    return tiles


def pieces_of(read, slab, r, target):
    return [(read(tile), lane, target + first) for tile, lane, first, _ in SLOTS[slab, r]]


def row_kernel(grid_ref, table_ref, out_ref, x_ref, xs, held, sem):
    chunk = 256
    count = COLUMNS // chunk
    grid_copy = pltpu.make_async_copy(grid_ref, x_ref, sem.at[4 * count])
    grid_copy.start()
    copies = {}
    for parity in range(2):
        for k in range(count):
            for part in range(2):
                copy = pltpu.make_async_copy(
                    table_ref.at[parity, part, :, pl.ds(k * chunk, chunk)],
                    held.at[parity, part, :, pl.ds(k * chunk, chunk)],
                    sem.at[(parity * count + k) * 2 + part],
                )
                copy.start()
                copies[parity, k, part] = copy
    xs[...] = jnp.zeros_like(xs)
    grid_copy.wait()
    for slab in range(2):
        xs[slab * PITCH : slab * PITCH + ROWS, :N] = x_ref[:, slab, :]
    full = xs[...]
    turned = pltpu.roll(full, full.shape[1] - HALF, 1)
    for parity in range(2):
        value = (full + turned if parity == 0 else full - turned)[:, :HALF]
        high, low = halves(value)
        both = jnp.concatenate([high, low], axis=0)
        results = []
        for k in range(count):
            copies[parity, k, 0].wait()
            copies[parity, k, 1].wait()
            columns = slice(k * chunk, (k + 1) * chunk)
            main = dot(both, held[parity, 0, :, columns])
            results.append(main[:PAIR] + main[PAIR:] + dot(high, held[parity, 1, :, columns]))
            for place in range(SIDE):
                if place // GROUP * 128 // chunk != k:
                    continue
                start = place // GROUP * 128 % chunk

                def read(slab, r):
                    rows = slice(slab * PITCH + 8 * r, slab * PITCH + 8 * r + 8)
                    return results[k][rows, start : start + 128], place % GROUP * WIDTH

                for tile, values in enumerate(packed(read)):
                    out_ref[parity * SIDE + place, 8 * tile : 8 * tile + 8, :] = values


def damp_kernel(lane_ref, out_ref):
    wave_square = lane_ref[0:1, :]
    limit = lane_ref[1:2, :]
    order = lane_ref[2:3, :]
    strength = lane_ref[3:4, :]
    for residue in range(4):
        m = lax.broadcasted_iota(jnp.int32, (QUARTER, 128), 0)
        q = 4 * m + residue
        wave = jnp.where(q < HALF, q, q - N).astype(jnp.float32)
        radius = (wave_square + wave * wave) / (0.5 * N) ** 2
        square = radius * radius
        powered = jnp.where(
            order == 1.0,
            radius,
            jnp.where(order == 2.0, square, jnp.where(order == 3.0, square * radius, square * square)),
        )
        inside = (jnp.abs(wave) <= limit).astype(jnp.float32)
        out_ref[residue] = inside / (1.0 + strength * powered)


def column_kernel(in_ref, damp_ref, lane_ref, forward_ref, back_ref, out_ref, energy_ref, held_forward, held_back, sem):
    copies = []
    for residue in range(4):
        copies.append(pltpu.make_async_copy(forward_ref.at[residue], held_forward.at[residue], sem.at[residue]))
    for residue in range(4):
        copies.append(pltpu.make_async_copy(back_ref.at[residue], held_back.at[residue], sem.at[4 + residue]))
    for copy in copies:
        copy.start()
    spot = lane_index(8) % 64
    packs_top = lane_ref[:, :][5:6, :] > 0.5
    to_top = (spot == WIDTH) & packs_top
    cleared = ((spot == WAVES) | (spot == WIDTH + WAVES)) & packs_top
    from_top = (spot == WAVES) & packs_top

    def turned(values):
        forward = pltpu.roll(values, 128 - WAVES, 1)
        backward = pltpu.roll(values, WAVES, 1)
        rows = lane_index(values.shape[0]) % 64
        real = (rows < WAVES) | (rows == WIDTH)
        return jnp.where(real, forward, -backward)

    def weights(values, other):
        return jnp.concatenate(
            [jnp.concatenate(halves(values), axis=1), jnp.concatenate(halves(other), axis=1)], axis=0
        )

    def folded(result):
        count = result.shape[0] // 2
        total = result[:count] + result[count:]
        return total[:, :128] + total[:, 128:]

    quarters = []
    for quarter in range(4):
        tiles = []
        for peer in range(quarter * PEERS // 4, (quarter + 1) * PEERS // 4):
            read = lambda tile: in_ref[peer, 8 * tile : 8 * tile + 8, :]
            for r in range(PITCH // 8):
                tile = gather_lanes(pieces_of(read, 0, r, 0) + pieces_of(read, 1, r, 64))
                tile = jnp.where(to_top, pltpu.roll(tile, WAVES, 1), jnp.where(cleared, 0.0, tile))
                tiles.append(tile)
        quarters.append(jnp.concatenate(tiles, axis=0))
    c, d = quarters[0] + quarters[2], quarters[1] + quarters[3]
    a, b = quarters[0] - quarters[2], quarters[1] - quarters[3]
    turned_c, turned_d, turned_a, turned_b = turned(c), turned(d), turned(a), turned(b)
    inputs = [
        (c + d, turned_c + turned_d),
        (a + turned_b, turned_a - b),
        (c - d, turned_c - turned_d),
        (a - turned_b, turned_a + b),
    ]
    energy = jnp.zeros((1, 128), jnp.float32)
    parts = [None] * 4
    damped = [None] * 4
    for residue in range(4):
        copies[residue].wait()
        spectrum = folded(dot(held_forward[residue], weights(*inputs[residue])))
        damped[residue] = spectrum * damp_ref[residue]
        energy = energy + jnp.sum(damped[residue] * damped[residue], axis=0, keepdims=True)
    for residue in range(4):
        copies[4 + residue].wait()
        parts[residue] = folded(dot(held_back[residue], weights(damped[residue], turned(damped[residue]))))
    even, odd = parts[0] + parts[2], parts[1] + parts[3]
    even_less, odd_less = parts[0] - parts[2], turned(parts[1] - parts[3])
    grids = [even + odd, even_less - odd_less, even - odd, even_less + odd_less]
    for quarter in range(4):
        for k in range(PEERS // 4):
            fixed = {}
            for r in range(PITCH // 8):
                tile = grids[quarter][k * PITCH + 8 * r : k * PITCH + 8 * r + 8]
                fixed[r] = jnp.where(from_top, pltpu.roll(tile, 128 - WAVES, 1), tile)
            for tile, values in enumerate(packed(lambda slab, r: (fixed[r], 64 * slab))):
                out_ref[quarter * (PEERS // 4) + k, 8 * tile : 8 * tile + 8, :] = values
    energy = energy * lane_ref[4:5, :]
    lane = lane_index(1)
    first = jnp.sum(jnp.where(lane < 64, energy, 0.0), axis=1, keepdims=True)
    second = jnp.sum(jnp.where(lane < 64, 0.0, energy), axis=1, keepdims=True)
    weighted = jnp.sum(energy * lane_ref[6:7, :], axis=1, keepdims=True)
    row = jnp.where(lane == 0, first, jnp.where(lane == 1, second, jnp.where(lane == 2, weighted, 0.0)))
    energy_ref[...] = jnp.broadcast_to(row, energy_ref.shape)


def back_kernel(in_ref, table_ref, out_ref, held, sem):
    copies = {}
    for parity in range(2):
        for part in range(2):
            copy = pltpu.make_async_copy(
                table_ref.at[parity, part], held.at[parity, part], sem.at[parity * 2 + part]
            )
            copy.start()
            copies[parity, part] = copy
    parts = []
    for parity in range(2):
        rows = []
        for slab in range(2):
            for r in range(PITCH // 8):
                columns = []
                for v in range(COLUMNS // 128):
                    pieces = []
                    for place in range(v * GROUP, min((v + 1) * GROUP, SIDE)):
                        read = lambda tile: in_ref[parity * SIDE + place, 8 * tile : 8 * tile + 8, :]
                        pieces += pieces_of(read, slab, r, place % GROUP * WIDTH)
                    columns.append(gather_lanes(pieces))
                rows.append(jnp.concatenate(columns, axis=1))
        high, low = halves(jnp.concatenate(rows, axis=0))
        copies[parity, 0].wait()
        main = dot(jnp.concatenate([high, low], axis=0), held[parity, 0])
        copies[parity, 1].wait()
        parts.append(main[:PAIR] + main[PAIR:] + dot(high, held[parity, 1]))
    lower, upper = parts[0] + parts[1], parts[0] - parts[1]
    for slab in range(2):
        rows = slice(slab * PITCH, slab * PITCH + ROWS)
        out_ref[:, slab, :HALF] = lower[rows]
        out_ref[:, slab, HALF:] = upper[rows]


def grant(mebibytes):
    return pltpu.CompilerParams(vmem_limit_bytes=mebibytes << 20)


def in_hbm(array):
    return pltpu.with_memory_space_constraint(array, pltpu.HBM)


VMEM = pl.BlockSpec(memory_space=pltpu.VMEM)
HBM = pl.BlockSpec(memory_space=pltpu.HBM)


def lane_values(place, truncation_limit, diffusion_order, diffusion_strength, mass_weight):
    parity, spot = place // SIDE, place % SIDE
    chosen = jnp.where(parity == 0, truncation_limit[0:HALF:2], truncation_limit[1:HALF:2])
    limits = lax.dynamic_slice(chosen, (spot * WAVES,), (WAVES,))
    slots = jnp.arange(64, dtype=jnp.int32)
    wave = jnp.where(slots < WIDTH, 2 * (spot * WAVES + slots % WAVES) + parity, HALF)
    top = (slots == WIDTH) | (slots == WIDTH + WAVES)
    weight = jnp.where(wave % HALF == 0, 1.0, 2.0) / float(N) ** 4
    weight = jnp.where((slots < WIDTH) | (top & (place == 0)), weight, 0.0)
    limits = jnp.concatenate(
        [limits, limits, jnp.broadcast_to(truncation_limit[HALF], (64 - WIDTH,))]
    ).astype(jnp.float32)
    wave = wave.astype(jnp.float32)
    rows = [
        jnp.tile(wave * wave, 2),
        jnp.tile(limits, 2),
        jnp.repeat(diffusion_order.astype(jnp.float32), 64),
        jnp.repeat(diffusion_strength, 64),
        jnp.tile(weight, 2),
        jnp.broadcast_to((place == 0).astype(jnp.float32), (128,)),
        jnp.repeat(mass_weight, 64),
        jnp.zeros((128,), jnp.float32),
    ]
    return jnp.stack(rows)


def local(grid_field, truncation_limit, diffusion_order, diffusion_strength, mass_weight):
    row_forward, row_back = row_tables()
    column_forward, column_back = column_tables()
    block = jax.ShapeDtypeStruct((PEERS, 24, 128), jnp.float32)
    levels = lax.axis_size("lev")
    everyone = levels * PEERS
    sent = pl.pallas_call(
        row_kernel,
        out_shape=block,
        in_specs=[HBM, HBM],
        out_specs=VMEM,
        scratch_shapes=[
            pltpu.VMEM((ROWS, 2, N), jnp.float32),
            pltpu.VMEM((PAIR, 1280), jnp.float32),
            pltpu.VMEM(row_forward.shape, jnp.bfloat16),
            pltpu.SemaphoreType.DMA((4 * COLUMNS // 256 + 1,)),
        ],
        compiler_params=grant(14),
        name="row_forward",
    )(in_hbm(grid_field.transpose(1, 0, 2)), in_hbm(jnp.asarray(row_forward)))
    received = lax.all_to_all(sent, "wav", split_axis=0, concat_axis=0, tiled=True)

    lanes = lane_values(
        lax.axis_index("wav"), truncation_limit, diffusion_order, diffusion_strength, mass_weight
    )
    damp = pl.pallas_call(
        damp_kernel,
        out_shape=jax.ShapeDtypeStruct((4, QUARTER, 128), jnp.float32),
        in_specs=[VMEM],
        out_specs=VMEM,
        compiler_params=grant(4),
        cost_estimate=pl.CostEstimate(flops=20_000_000, bytes_accessed=600_000, transcendentals=0),
        name="damping",
    )(lanes)
    back, energy = pl.pallas_call(
        column_kernel,
        out_shape=(block, jax.ShapeDtypeStruct((everyone, 128), jnp.float32)),
        in_specs=[VMEM] * 3 + [HBM] * 2,
        out_specs=(VMEM, VMEM),
        scratch_shapes=[
            pltpu.VMEM(column_forward.shape, jnp.bfloat16),
            pltpu.VMEM(column_back.shape, jnp.bfloat16),
            pltpu.SemaphoreType.DMA((8,)),
        ],
        compiler_params=grant(24),
        name="column",
    )(received, damp, lanes, in_hbm(jnp.asarray(column_forward)), in_hbm(jnp.asarray(column_back)))
    returned = lax.all_to_all(back, "wav", split_axis=0, concat_axis=0, tiled=True)
    shares = lax.all_to_all(energy, ("lev", "wav"), split_axis=0, concat_axis=0, tiled=True)
    row_back_call = pl.pallas_call(
        back_kernel,
        out_shape=jax.ShapeDtypeStruct((ROWS, 2, N), jnp.float32),
        in_specs=[VMEM, HBM],
        out_specs=VMEM,
        scratch_shapes=[
            pltpu.VMEM(row_back.shape, jnp.bfloat16),
            pltpu.SemaphoreType.DMA((4,)),
        ],
        compiler_params=grant(14),
        cost_estimate=pl.CostEstimate(flops=2_000_000_000, bytes_accessed=6_000_000, transcendentals=0),
        name="row_back",
    )
    filtered = row_back_call(returned, in_hbm(jnp.asarray(row_back)))
    mine = lax.dynamic_slice(shares, (lax.axis_index("lev") * PEERS, 0), (PEERS, 2))
    energies = jnp.sum(mine, axis=0)
    total_energy = jnp.sum(shares[:, 2]) / (2 * levels)
    return filtered.transpose(1, 0, 2), energies, total_energy


def solution(mesh):
    placed = (P("lev", "wav", None), P(), P("lev"), P("lev"), P("lev"))
    return jax.shard_map(
        local,
        mesh=mesh,
        in_specs=placed,
        out_specs=(P("lev", "wav", None), P("lev"), P()),
        check_vma=False,
    )
```

```python
import functools
import math

import jax
import jax.numpy as jnp
import ml_dtypes
import numpy as np
from jax import lax
from jax.experimental import pallas as pl
from jax.experimental.pallas import tpu as pltpu
from jax.sharding import PartitionSpec as P

N = 1216
HALF = N // 2
QUARTER = N // 4
PEERS = 32
ROWS = N // PEERS
PITCH = 40
WAVES = HALF // PEERS
WIDTH = 2 * WAVES
SIDE = PEERS // 2
GROUP = 3
COLUMNS = -(-SIDE // GROUP) * 128
BLOCK = PEERS // 4 * PITCH
PAIR = 2 * PITCH
SLOTS = {
    (0, 0): [(0, 0, 0, WIDTH)],
    (0, 1): [(1, 0, 0, WIDTH)],
    (0, 2): [(2, 0, 0, WIDTH)],
    (1, 0): [(0, 38, 0, WIDTH)],
    (1, 1): [(1, 38, 0, WIDTH)],
    (1, 2): [(2, 38, 0, WIDTH)],
    (0, 3): [(0, 76, 0, WIDTH)],
    (1, 3): [(1, 76, 0, WIDTH)],
    (0, 4): [(2, 76, 0, WIDTH)],
    (1, 4): [(0, 114, 0, 14), (1, 114, 14, 14), (2, 114, 28, 10)],
}

SHARE_ROW, SHARE_LANE = 16 + ROWS - 32, 76


def split(table):
    high = table.astype(ml_dtypes.bfloat16)
    low = (table - high.astype(np.float64)).astype(ml_dtypes.bfloat16)
    return high, low


def angle(product):
    return (product % N).astype(np.float64) * (2.0 * math.pi / N)


@functools.cache
def row_tables():
    j = np.arange(HALF)
    forward = np.zeros((2, HALF, COLUMNS))
    back = np.zeros((2, COLUMNS, HALF))
    for parity in range(2):
        for place in range(SIDE):
            wave = 2 * (place * WAVES + np.arange(WAVES)) + parity
            theta = angle(j[:, None] * wave[None, :])
            cosine, sine = np.cos(theta), -np.sin(theta)
            weight = np.where(wave == 0, 1.0, 2.0)
            if wave[0] == 0:
                sine[:, 0] = np.cos(angle(j * HALF))
            both = np.concatenate([cosine, sine], axis=1)
            start = place // GROUP * 128 + place % GROUP * WIDTH
            forward[parity, :, start : start + WIDTH] = both
            back[parity, start : start + WIDTH, :] = (
                both * np.concatenate([weight, weight]) / float(N) ** 2
            ).T
    return (
        np.stack([np.stack(split(t)) for t in forward]),
        np.stack([np.stack(split(t)) for t in back]),
    )


@functools.cache
def column_tables():
    place = np.full((PEERS // 4, PITCH), -1, np.int64)
    place[:, :ROWS] = np.arange(QUARTER).reshape(PEERS // 4, ROWS)
    place = place.reshape(-1)
    used = (place >= 0).astype(np.float64)
    spot = np.maximum(place, 0)
    m = np.arange(QUARTER)
    forward, back = [], []
    for residue in range(4):
        theta = angle((4 * m + residue)[:, None] * spot[None, :])
        cosine, sine = np.cos(theta) * used, np.sin(theta) * used
        forward.append(np.concatenate(split(np.concatenate([cosine, sine], axis=1)), axis=0))
        back.append(np.concatenate(split(np.concatenate([cosine.T, -sine.T], axis=1)), axis=0))
    return np.stack(forward), np.stack(back)


def dot(left, right):
    return lax.dot_general(left, right, (((1,), (0,)), ((), ())), preferred_element_type=jnp.float32)


def halves(values):
    high = values.astype(jnp.bfloat16)
    low = (values - high.astype(jnp.float32)).astype(jnp.bfloat16)
    return high, low


def lane_index(rows):
    return lax.broadcasted_iota(jnp.int32, (rows, 128), 1)


def turn(values, shift):
    return values if shift % 128 == 0 else pltpu.roll(values, shift % 128, 1)


def gather_lanes(pieces):
    lane = lane_index(8)
    result = None
    for values, source, target in pieces:
        turned = turn(values, target - source)
        result = turned if result is None else jnp.where(lane >= target, turned, result)
    return result


def packed(read):
    tiles = []
    for tile in range(3):
        pieces = []
        for (slab, r), slots in SLOTS.items():
            for where, lane, first, _ in slots:
                if where == tile:
                    values, start = read(slab, r)
                    pieces.append((values, start + first, lane))
        tiles.append(gather_lanes(sorted(pieces, key=lambda p: p[2])))
    return tiles


def pieces_of(read, slab, r, target):
    return [(read(tile), lane, target + first) for tile, lane, first, _ in SLOTS[slab, r]]


def row_kernel(
    grid_ref, table_ref, limit_in, order_in, strength_in, mass_in, out_ref, lane_ref, damp_ref,
    limit_ref, order_ref, strength_ref, mass_ref, x_ref, xs, both, held, sem, small_sem,
):
    chunk = 256
    count = COLUMNS // chunk
    inside = chunk // 128 * GROUP

    def table_copy(step):
        columns = pl.ds(pl.multiple_of(step % count * chunk, chunk), chunk)
        return pltpu.make_async_copy(
            table_ref.at[step // count, :, :, columns], held.at[step], sem.at[step]
        )

    small_copies = [
        pltpu.make_async_copy(source, target, small_sem.at[k])
        for k, (source, target) in enumerate(
            [(limit_in, limit_ref), (order_in, order_ref), (strength_in, strength_ref), (mass_in, mass_ref)]
        )
    ]
    for copy in small_copies:
        copy.start()
    grid_copy = pltpu.make_async_copy(grid_ref, x_ref, sem.at[2 * count])
    grid_copy.start()
    for step in range(2 * count):
        table_copy(step).start()
    lane_ref[...] = jnp.zeros_like(lane_ref)
    for copy in small_copies:
        copy.wait()
    fill_lanes(lane_ref, limit_ref, order_ref, strength_ref, mass_ref)
    fill_damping(lane_ref, damp_ref)
    xs[...] = jnp.zeros_like(xs)
    grid_copy.wait()
    for slab in range(2):
        xs[slab * PITCH : slab * PITCH + ROWS, :N] = x_ref[:, slab, :]
    full = xs[...]
    turned = pltpu.roll(full, full.shape[1] - HALF, 1)
    for parity in range(2):
        value = (full + turned if parity == 0 else full - turned)[:, :HALF]
        high, low = halves(value)
        both[parity, :PAIR] = high
        both[parity, PAIR:] = low

    @pl.loop(0, 2 * count)
    def _(step):
        parity, k = step // count, step % count
        table_copy(step).wait()
        main = dot(both[parity], held[step, 0])
        result = main[:PAIR] + main[PAIR:] + dot(both[parity, :PAIR], held[step, 1])
        for spot in range(inside):

            def store(spot=spot):
                start = spot // GROUP * 128

                def read(slab, r):
                    rows = slice(slab * PITCH + 8 * r, slab * PITCH + 8 * r + 8)
                    return result[rows, start : start + 128], spot % GROUP * WIDTH

                for tile, values in enumerate(packed(read)):
                    out_ref[parity * SIDE + k * inside + spot, 8 * tile : 8 * tile + 8, :] = values

            if spot + (count - 1) * inside < SIDE:
                store()
            else:
                pl.when(k < count - 1)(store)


def fill_lanes(lane_ref, limit_ref, order_ref, strength_ref, mass_ref):
    place = lax.axis_index("wav")
    parity, spot = place // SIDE, place % SIDE
    lane = lane_index(1)
    column = lane % 64
    slot = jnp.where(column < WAVES, column, column - WAVES)
    regular = column < WIDTH
    wave = jnp.where(regular, 2 * (spot * WAVES + slot) + parity, HALF)
    limit = jnp.broadcast_to(limit_ref[HALF], (1, 128))
    for k in range(WAVES):
        limit = jnp.where(regular & (slot == k), limit_ref[2 * (spot * WAVES + k) + parity], limit)
    weight = jnp.where((wave == 0) | (wave == HALF), 1.0, 2.0) / float(N) ** 4
    top = ((column == WIDTH) | (column == WIDTH + WAVES)) & (place == 0)
    first = lane < 64
    wave = wave.astype(jnp.float32)
    rows = [
        wave * wave,
        limit.astype(jnp.float32),
        jnp.where(first, order_ref[0], order_ref[1]).astype(jnp.float32),
        jnp.where(first, strength_ref[0], strength_ref[1]),
        jnp.where(regular | top, weight, 0.0),
        jnp.where(jnp.broadcast_to(place, (1, 128)) == 0, 1.0, 0.0),
        jnp.where(first, mass_ref[0], mass_ref[1]),
    ]
    for k, row in enumerate(rows):
        lane_ref[k : k + 1, :] = row


def fill_damping(lane_ref, damp_ref):
    wave_square = lane_ref[0:1, :]
    limit = lane_ref[1:2, :]
    order = lane_ref[2:3, :]
    strength = lane_ref[3:4, :]

    @pl.loop(0, 4)
    def _(residue):
        q = 4 * lax.broadcasted_iota(jnp.int32, (QUARTER, 128), 0) + residue
        wave = jnp.where(q < HALF, q, q - N).astype(jnp.float32)
        radius = (wave_square + wave * wave) / (0.5 * N) ** 2
        square = radius * radius
        powered = jnp.where(
            order == 1.0,
            radius,
            jnp.where(order == 2.0, square, jnp.where(order == 3.0, square * radius, square * square)),
        )
        damp_ref[residue] = jnp.where(jnp.abs(wave) <= limit, 1.0 / (1.0 + strength * powered), 0.0)


def column_kernel(
    in_ref, damp_ref, lane_ref, forward_ref, back_ref, out_ref, held_forward, held_back, mixed, parts, total, sem
):
    def forward_copy(residue):
        return pltpu.make_async_copy(forward_ref.at[residue], held_forward.at[residue], sem.at[residue])

    def back_copy(residue):
        return pltpu.make_async_copy(back_ref.at[residue], held_back.at[residue], sem.at[4 + residue])

    for residue in range(4):
        forward_copy(residue).start()
        back_copy(residue).start()
    packs_top = lane_ref[5:6, :] > 0.5
    peers = 2
    rows = peers * PITCH

    def turned(values):
        forward = pltpu.roll(values, 128 - WAVES, 1)
        backward = pltpu.roll(values, WAVES, 1)
        spot = lane_index(values.shape[0]) % 64
        return jnp.where((spot < WAVES) | (spot == WIDTH), forward, -backward)

    def folded(result):
        count = result.shape[0] // 2
        both = result[:count] + result[count:]
        return both[:, :128] + both[:, 128:]

    @pl.loop(0, PEERS // 4 // peers)
    def _(step):
        spot = lane_index(8) % 64
        to_top = (spot == WIDTH) & packs_top
        cleared = ((spot == WAVES) | (spot == WIDTH + WAVES)) & packs_top
        quarters = []
        for quarter in range(4):
            tiles = []
            for k in range(peers):
                peer = quarter * (PEERS // 4) + step * peers + k
                read = lambda tile: in_ref[peer, 8 * tile : 8 * tile + 8, :]
                for r in range(PITCH // 8):
                    tile = gather_lanes(pieces_of(read, 0, r, 0) + pieces_of(read, 1, r, 64))
                    tile = jnp.where(to_top, pltpu.roll(tile, WAVES, 1), jnp.where(cleared, 0.0, tile))
                    tiles.append(tile)
            quarters.append(jnp.concatenate(tiles, axis=0))
        c, d = quarters[0] + quarters[2], quarters[1] + quarters[3]
        a, b = quarters[0] - quarters[2], quarters[1] - quarters[3]
        turned_c, turned_d, turned_a, turned_b = turned(c), turned(d), turned(a), turned(b)
        inputs = [
            (c + d, turned_c + turned_d),
            (a + turned_b, turned_a - b),
            (c - d, turned_c - turned_d),
            (a - turned_b, turned_a + b),
        ]
        start = pl.multiple_of(step * rows, rows)
        for residue in range(4):
            for k in range(2):
                mixed[residue, pl.ds(k * BLOCK + start, rows), :] = jnp.concatenate(
                    halves(inputs[residue][k]), axis=1
                )

    total[...] = jnp.zeros_like(total)

    @pl.loop(0, 4)
    def _(residue):
        forward_copy(residue).wait()
        spectrum = folded(dot(held_forward[residue], mixed[residue]))
        damped = spectrum * damp_ref[residue]
        total[...] += jnp.sum((damped * damped).reshape(QUARTER // 8, 8, 128), axis=0)
        weights = jnp.concatenate(
            [jnp.concatenate(halves(damped), axis=1), jnp.concatenate(halves(turned(damped)), axis=1)], axis=0
        )
        back_copy(residue).wait()
        parts[residue] = folded(dot(held_back[residue], weights))

    @pl.loop(0, PEERS // 4 // peers)
    def _(step):
        start = pl.multiple_of(step * rows, rows)
        part = [parts[residue, pl.ds(start, rows), :] for residue in range(4)]
        even, odd = part[0] + part[2], part[1] + part[3]
        even_less, odd_less = part[0] - part[2], turned(part[1] - part[3])
        from_top = (lane_index(8) % 64 == WAVES) & packs_top
        for quarter, grid in enumerate([even + odd, even_less - odd_less, even - odd, even_less + odd_less]):
            for k in range(peers):
                fixed = {}
                for r in range(PITCH // 8):
                    tile = grid[k * PITCH + 8 * r : k * PITCH + 8 * r + 8]
                    fixed[r] = jnp.where(from_top, pltpu.roll(tile, 128 - WAVES, 1), tile)
                for tile, values in enumerate(packed(lambda slab, r: (fixed[r], 64 * slab))):
                    out_ref[quarter * (PEERS // 4) + step * peers + k, 8 * tile : 8 * tile + 8, :] = values

    energy = jnp.sum(total[...], axis=0, keepdims=True) * lane_ref[4:5, :]
    lane = lane_index(1)
    first = jnp.sum(jnp.where(lane < 64, energy, 0.0), axis=1, keepdims=True)
    second = jnp.sum(jnp.where(lane < 64, 0.0, energy), axis=1, keepdims=True)
    weighted = jnp.sum(energy * lane_ref[6:7, :], axis=1, keepdims=True)
    row = jnp.where(
        lane == SHARE_LANE, first, jnp.where(lane == SHARE_LANE + 1, second, weighted)
    )
    shared = (lane >= SHARE_LANE) & (lane < SHARE_LANE + 3)

    @pl.loop(0, PEERS)
    def _(peer):
        kept = out_ref[peer, SHARE_ROW : SHARE_ROW + 1, :]
        out_ref[peer, SHARE_ROW : SHARE_ROW + 1, :] = jnp.where(shared, row, kept)


def share_kernel(in_ref, out_ref):
    total = in_ref[0, SHARE_ROW : SHARE_ROW + 1, :]
    for peer in range(1, PEERS):
        total = total + in_ref[peer, SHARE_ROW : SHARE_ROW + 1, :]
    out_ref[...] = jnp.broadcast_to(pltpu.roll(total, 128 - SHARE_LANE, 1), out_ref.shape)


def back_kernel(in_ref, table_ref, out_ref, held, both, sem):
    def table_copy(parity):
        return pltpu.make_async_copy(table_ref.at[parity], held.at[parity], sem.at[parity])

    for parity in range(2):
        table_copy(parity).start()
    count = COLUMNS // 128

    @pl.loop(0, 2 * count)
    def _(step):
        parity, v = step // count, step % count
        tiles = []
        for slab in range(2):
            for r in range(PITCH // 8):
                pieces = []
                for spot in range(GROUP):
                    peer = jnp.minimum(parity * SIDE + v * GROUP + spot, PEERS - 1)
                    read = lambda tile: in_ref[peer, 8 * tile : 8 * tile + 8, :]
                    pieces += pieces_of(read, slab, r, spot * WIDTH)
                tiles.append(gather_lanes(pieces))
        high, low = halves(jnp.concatenate(tiles, axis=0))
        columns = pl.ds(pl.multiple_of(v * 128, 128), 128)
        both[parity, :PAIR, columns] = high
        both[parity, PAIR:, columns] = low

    parts = []
    for parity in range(2):
        table_copy(parity).wait()
        main = dot(both[parity], held[parity, 0])
        parts.append(main[:PAIR] + main[PAIR:] + dot(both[parity, :PAIR], held[parity, 1]))
    lower, upper = parts[0] + parts[1], parts[0] - parts[1]
    for slab in range(2):
        rows = slice(slab * PITCH, slab * PITCH + ROWS)
        out_ref[:, slab, :HALF] = lower[rows]
        out_ref[:, slab, HALF:] = upper[rows]


def grant(mebibytes):
    return pltpu.CompilerParams(vmem_limit_bytes=mebibytes << 20)


def in_hbm(array):
    return pltpu.with_memory_space_constraint(array, pltpu.HBM)


VMEM = pl.BlockSpec(memory_space=pltpu.VMEM)
HBM = pl.BlockSpec(memory_space=pltpu.HBM)


def local(grid_field, truncation_limit, diffusion_order, diffusion_strength, mass_weight):
    row_forward, row_back = row_tables()
    column_forward, column_back = column_tables()
    block = jax.ShapeDtypeStruct((PEERS, 24, 128), jnp.float32)
    levels = lax.axis_size("lev")
    row_steps = 2 * COLUMNS // 256
    sent, lanes, damp = pl.pallas_call(
        row_kernel,
        out_shape=(
            block,
            jax.ShapeDtypeStruct((8, 128), jnp.float32),
            jax.ShapeDtypeStruct((4, QUARTER, 128), jnp.float32),
        ),
        in_specs=[HBM] * 6,
        out_specs=(VMEM, VMEM, VMEM),
        scratch_shapes=[
            pltpu.SMEM((N,), jnp.int32),
            pltpu.SMEM((2,), jnp.int32),
            pltpu.SMEM((2,), jnp.float32),
            pltpu.SMEM((2,), jnp.float32),
            pltpu.VMEM((ROWS, 2, N), jnp.float32),
            pltpu.VMEM((PAIR, 1280), jnp.float32),
            pltpu.VMEM((2, 2 * PAIR, HALF), jnp.bfloat16),
            pltpu.VMEM((row_steps, 2, HALF, 256), jnp.bfloat16),
            pltpu.SemaphoreType.DMA((row_steps + 1,)),
            pltpu.SemaphoreType.DMA((4,)),
        ],
        compiler_params=grant(14),
        name="row_forward",
    )(
        in_hbm(grid_field.transpose(1, 0, 2)),
        in_hbm(jnp.asarray(row_forward)),
        in_hbm(truncation_limit),
        in_hbm(diffusion_order),
        in_hbm(diffusion_strength),
        in_hbm(mass_weight),
    )
    received = lax.all_to_all(sent, "wav", split_axis=0, concat_axis=0, tiled=True)
    back = pl.pallas_call(
        column_kernel,
        out_shape=block,
        in_specs=[VMEM] * 3 + [HBM] * 2,
        out_specs=VMEM,
        scratch_shapes=[
            pltpu.VMEM(column_forward.shape, jnp.bfloat16),
            pltpu.VMEM(column_back.shape, jnp.bfloat16),
            pltpu.VMEM((4, 2 * BLOCK, 256), jnp.bfloat16),
            pltpu.VMEM((4, BLOCK, 128), jnp.float32),
            pltpu.VMEM((8, 128), jnp.float32),
            pltpu.SemaphoreType.DMA((8,)),
        ],
        compiler_params=grant(16),
        name="column",
    )(received, damp, lanes, in_hbm(jnp.asarray(column_forward)), in_hbm(jnp.asarray(column_back)))
    returned = lax.all_to_all(back, "wav", split_axis=0, concat_axis=0, tiled=True)
    shares = pl.pallas_call(
        share_kernel,
        out_shape=jax.ShapeDtypeStruct((levels, 128), jnp.float32),
        in_specs=[VMEM],
        out_specs=VMEM,
        compiler_params=grant(2),
        name="share",
    )(returned)
    everyone = lax.all_to_all(shares, "lev", split_axis=0, concat_axis=0, tiled=True)
    row_back_call = pl.pallas_call(
        back_kernel,
        out_shape=jax.ShapeDtypeStruct((ROWS, 2, N), jnp.float32),
        in_specs=[VMEM, HBM],
        out_specs=VMEM,
        scratch_shapes=[
            pltpu.VMEM(row_back.shape, jnp.bfloat16),
            pltpu.VMEM((2, 2 * PAIR, COLUMNS), jnp.bfloat16),
            pltpu.SemaphoreType.DMA((2,)),
        ],
        compiler_params=grant(14),
        cost_estimate=pl.CostEstimate(flops=2_000_000_000, bytes_accessed=6_000_000, transcendentals=0),
        name="row_back",
    )
    filtered = row_back_call(returned, in_hbm(jnp.asarray(row_back)))
    energies = shares[0, :2]
    total_energy = jnp.sum(everyone[:, 2]) / (2 * levels)
    return filtered.transpose(1, 0, 2), energies, total_energy


def solution(mesh):
    placed = (P("lev", "wav", None), P(), P("lev"), P("lev"), P("lev"))
    return jax.shard_map(
        local,
        mesh=mesh,
        in_specs=placed,
        out_specs=(P("lev", "wav", None), P("lev"), P()),
        check_vma=False,
    )
```

```python
import functools
import math

import jax
import jax.numpy as jnp
import ml_dtypes
import numpy as np
from jax import lax
from jax.experimental import pallas as pl
from jax.experimental.pallas import tpu as pltpu
from jax.sharding import PartitionSpec as P

N = 1216
HALF = N // 2
QUARTER = N // 4
PEERS = 32
ROWS = N // PEERS
PITCH = 40
WAVES = HALF // PEERS
WIDTH = 2 * WAVES
SIDE = PEERS // 2
GROUP = 3
COLUMNS = -(-SIDE // GROUP) * 128
BLOCK = PEERS // 4 * PITCH
PAIR = 2 * PITCH
SLOTS = {
    (0, 0): [(0, 0, 0, WIDTH)],
    (0, 1): [(1, 0, 0, WIDTH)],
    (0, 2): [(2, 0, 0, WIDTH)],
    (1, 0): [(0, 38, 0, WIDTH)],
    (1, 1): [(1, 38, 0, WIDTH)],
    (1, 2): [(2, 38, 0, WIDTH)],
    (0, 3): [(0, 76, 0, WIDTH)],
    (1, 3): [(1, 76, 0, WIDTH)],
    (0, 4): [(2, 76, 0, WIDTH)],
    (1, 4): [(0, 114, 0, 14), (1, 114, 14, 14), (2, 114, 28, 10)],
}

SHARE_ROW, SHARE_LANE = 16 + ROWS - 32, 76


def split(table):
    high = table.astype(ml_dtypes.bfloat16)
    low = (table - high.astype(np.float64)).astype(ml_dtypes.bfloat16)
    return high, low


def angle(product):
    return (product % N).astype(np.float64) * (2.0 * math.pi / N)


@functools.cache
def row_tables():
    j = np.arange(HALF)
    forward = np.zeros((2, HALF, COLUMNS))
    back = np.zeros((2, COLUMNS, HALF))
    for parity in range(2):
        for place in range(SIDE):
            wave = 2 * (place * WAVES + np.arange(WAVES)) + parity
            theta = angle(j[:, None] * wave[None, :])
            cosine, sine = np.cos(theta), -np.sin(theta)
            weight = np.where(wave == 0, 1.0, 2.0)
            if wave[0] == 0:
                sine[:, 0] = np.cos(angle(j * HALF))
            both = np.concatenate([cosine, sine], axis=1)
            start = place // GROUP * 128 + place % GROUP * WIDTH
            forward[parity, :, start : start + WIDTH] = both
            back[parity, start : start + WIDTH, :] = (
                both * np.concatenate([weight, weight]) / float(N) ** 2
            ).T
    return (
        np.stack([np.stack(split(t)) for t in forward]),
        np.stack([np.stack(split(t)) for t in back]),
    )


@functools.cache
def column_tables():
    place = np.full((PEERS // 4, PITCH), -1, np.int64)
    place[:, :ROWS] = np.arange(QUARTER).reshape(PEERS // 4, ROWS)
    place = place.reshape(-1)
    used = (place >= 0).astype(np.float64)
    spot = np.maximum(place, 0)
    m = np.arange(QUARTER)
    forward, back = [], []
    for residue in range(4):
        theta = angle((4 * m + residue)[:, None] * spot[None, :])
        cosine, sine = np.cos(theta) * used, np.sin(theta) * used
        forward.append(np.concatenate(split(np.concatenate([cosine, sine], axis=1)), axis=0))
        back.append(np.concatenate(split(np.concatenate([cosine.T, -sine.T], axis=1)), axis=0))
    return np.stack(forward), np.stack(back)


def dot(left, right):
    return lax.dot_general(left, right, (((1,), (0,)), ((), ())), preferred_element_type=jnp.float32)


def halves(values):
    high = values.astype(jnp.bfloat16)
    low = (values - high.astype(jnp.float32)).astype(jnp.bfloat16)
    return high, low


def lane_index(rows):
    return lax.broadcasted_iota(jnp.int32, (rows, 128), 1)


def turn(values, shift):
    return values if shift % 128 == 0 else pltpu.roll(values, shift % 128, 1)


def gather_lanes(pieces):
    lane = lane_index(8)
    result = None
    for values, source, target in pieces:
        turned = turn(values, target - source)
        result = turned if result is None else jnp.where(lane >= target, turned, result)
    return result


def packed(read):
    tiles = []
    for tile in range(3):
        pieces = []
        for (slab, r), slots in SLOTS.items():
            for where, lane, first, _ in slots:
                if where == tile:
                    values, start = read(slab, r)
                    pieces.append((values, start + first, lane))
        tiles.append(gather_lanes(sorted(pieces, key=lambda p: p[2])))
    return tiles


def pieces_of(read, slab, r, target):
    return [(read(tile), lane, target + first) for tile, lane, first, _ in SLOTS[slab, r]]


def row_kernel(
    grid_ref, table_ref, limit_in, order_in, strength_in, mass_in, out_ref, lane_ref, damp_ref,
    limit_ref, order_ref, strength_ref, mass_ref, x_ref, xs, both, held, sem, small_sem,
):
    chunk = 256
    count = COLUMNS // chunk
    inside = chunk // 128 * GROUP

    def table_copy(step):
        columns = pl.ds(pl.multiple_of(step % count * chunk, chunk), chunk)
        return pltpu.make_async_copy(
            table_ref.at[step // count, :, :, columns], held.at[step], sem.at[step]
        )

    small_copies = [
        pltpu.make_async_copy(source, target, small_sem.at[k])
        for k, (source, target) in enumerate(
            [(limit_in, limit_ref), (order_in, order_ref), (strength_in, strength_ref), (mass_in, mass_ref)]
        )
    ]
    for copy in small_copies:
        copy.start()
    grid_copy = pltpu.make_async_copy(grid_ref, x_ref, sem.at[2 * count])
    grid_copy.start()
    for step in range(2 * count):
        table_copy(step).start()
    lane_ref[...] = jnp.zeros_like(lane_ref)
    for copy in small_copies:
        copy.wait()
    fill_lanes(lane_ref, limit_ref, order_ref, strength_ref, mass_ref)
    fill_damping(lane_ref, damp_ref)
    xs[...] = jnp.zeros_like(xs)
    grid_copy.wait()
    for slab in range(2):
        xs[slab * PITCH : slab * PITCH + ROWS, :N] = x_ref[:, slab, :]
    full = xs[...]
    turned = pltpu.roll(full, full.shape[1] - HALF, 1)
    for parity in range(2):
        value = (full + turned if parity == 0 else full - turned)[:, :HALF]
        high, low = halves(value)
        both[parity, :PAIR] = high
        both[parity, PAIR:] = low

    @pl.loop(0, 2 * count)
    def _(step):
        parity, k = step // count, step % count
        table_copy(step).wait()
        main = dot(both[parity], held[step, 0])
        result = main[:PAIR] + main[PAIR:] + dot(both[parity, :PAIR], held[step, 1])
        for spot in range(inside):

            def store(spot=spot):
                start = spot // GROUP * 128

                def read(slab, r):
                    rows = slice(slab * PITCH + 8 * r, slab * PITCH + 8 * r + 8)
                    return result[rows, start : start + 128], spot % GROUP * WIDTH

                for tile, values in enumerate(packed(read)):
                    out_ref[parity * SIDE + k * inside + spot, 8 * tile : 8 * tile + 8, :] = values

            if spot + (count - 1) * inside < SIDE:
                store()
            else:
                pl.when(k < count - 1)(store)


def fill_lanes(lane_ref, limit_ref, order_ref, strength_ref, mass_ref):
    place = lax.axis_index("wav")
    parity, spot = place // SIDE, place % SIDE
    lane = lane_index(1)
    column = lane % 64
    slot = jnp.where(column < WAVES, column, column - WAVES)
    regular = column < WIDTH
    wave = jnp.where(regular, 2 * (spot * WAVES + slot) + parity, HALF)
    limit = jnp.broadcast_to(limit_ref[HALF], (1, 128))
    for k in range(WAVES):
        limit = jnp.where(regular & (slot == k), limit_ref[2 * (spot * WAVES + k) + parity], limit)
    weight = jnp.where((wave == 0) | (wave == HALF), 1.0, 2.0) / float(N) ** 4
    top = ((column == WIDTH) | (column == WIDTH + WAVES)) & (place == 0)
    first = lane < 64
    wave = wave.astype(jnp.float32)
    rows = [
        wave * wave,
        limit.astype(jnp.float32),
        jnp.where(first, order_ref[0], order_ref[1]).astype(jnp.float32),
        jnp.where(first, strength_ref[0], strength_ref[1]),
        jnp.where(regular | top, weight, 0.0),
        jnp.where(jnp.broadcast_to(place, (1, 128)) == 0, 1.0, 0.0),
        jnp.where(first, mass_ref[0], mass_ref[1]),
    ]
    for k, row in enumerate(rows):
        lane_ref[k : k + 1, :] = row


def fill_damping(lane_ref, damp_ref):
    wave_square = lane_ref[0:1, :]
    limit = lane_ref[1:2, :]
    order = lane_ref[2:3, :]
    strength = lane_ref[3:4, :]

    @pl.loop(0, 4)
    def _(residue):
        q = 4 * lax.broadcasted_iota(jnp.int32, (QUARTER, 128), 0) + residue
        wave = jnp.where(q < HALF, q, q - N).astype(jnp.float32)
        radius = (wave_square + wave * wave) / (0.5 * N) ** 2
        square = radius * radius
        powered = jnp.where(
            order == 1.0,
            radius,
            jnp.where(order == 2.0, square, jnp.where(order == 3.0, square * radius, square * square)),
        )
        damp_ref[residue] = jnp.where(jnp.abs(wave) <= limit, 1.0 / (1.0 + strength * powered), 0.0)


def turned(values):
    forward = pltpu.roll(values, 128 - WAVES, 1)
    backward = pltpu.roll(values, WAVES, 1)
    spot = lane_index(values.shape[0]) % 64
    return jnp.where((spot < WAVES) | (spot == WIDTH), forward, -backward)


def folded(result):
    count = result.shape[0] // 2
    both = result[:count] + result[count:]
    return both[:, :128] + both[:, 128:]


def weights(values, other):
    return jnp.concatenate(
        [jnp.concatenate(halves(values), axis=1), jnp.concatenate(halves(other), axis=1)], axis=0
    )


def column_kernel(in_ref, damp_ref, lane_ref, table_ref, out_ref, share_ref):
    packs_top = lane_ref[5:6, :] > 0.5
    spot = lane_index(8) % 64
    to_top = (spot == WIDTH) & packs_top
    cleared = ((spot == WAVES) | (spot == WIDTH + WAVES)) & packs_top
    quarters = []
    for quarter in range(4):
        tiles = []
        for peer in range(quarter * PEERS // 4, (quarter + 1) * PEERS // 4):
            read = lambda tile: in_ref[peer, 8 * tile : 8 * tile + 8, :]
            for r in range(PITCH // 8):
                tile = gather_lanes(pieces_of(read, 0, r, 0) + pieces_of(read, 1, r, 64))
                tile = jnp.where(to_top, pltpu.roll(tile, WAVES, 1), jnp.where(cleared, 0.0, tile))
                tiles.append(tile)
        quarters.append(jnp.concatenate(tiles, axis=0))
    c, d = quarters[0] + quarters[2], quarters[1] + quarters[3]
    a, b = quarters[0] - quarters[2], quarters[1] - quarters[3]
    turned_c, turned_d, turned_a, turned_b = turned(c), turned(d), turned(a), turned(b)
    inputs = [
        (c + d, turned_c + turned_d),
        (a + turned_b, turned_a - b),
        (c - d, turned_c - turned_d),
        (a - turned_b, turned_a + b),
    ]
    energy = jnp.zeros((8, 128), jnp.float32)
    for residue in range(4):
        damped = folded(dot(table_ref[residue], weights(*inputs[residue]))) * damp_ref[residue]
        out_ref[residue] = damped
        energy = energy + jnp.sum((damped * damped).reshape(QUARTER // 8, 8, 128), axis=0)
    energy = jnp.sum(energy, axis=0, keepdims=True) * lane_ref[4:5, :]
    lane = lane_index(1)
    first = jnp.sum(jnp.where(lane < 64, energy, 0.0), axis=1, keepdims=True)
    second = jnp.sum(jnp.where(lane < 64, 0.0, energy), axis=1, keepdims=True)
    weighted = jnp.sum(energy * lane_ref[6:7, :], axis=1, keepdims=True)
    row = jnp.where(lane == 0, first, jnp.where(lane == 1, second, jnp.where(lane == 2, weighted, 0.0)))
    share_ref[...] = jnp.broadcast_to(row, share_ref.shape)


def column_back_kernel(in_ref, lane_ref, table_ref, out_ref, held, parts, sem):
    def table_copy(residue):
        return pltpu.make_async_copy(table_ref.at[residue], held.at[residue], sem.at[residue])

    for residue in range(4):
        table_copy(residue).start()
    packs_top = lane_ref[5:6, :] > 0.5
    peers = 2
    rows = peers * PITCH

    @pl.loop(0, 4)
    def _(residue):
        damped = in_ref[residue]
        table_copy(residue).wait()
        parts[residue] = folded(dot(held[residue], weights(damped, turned(damped))))

    @pl.loop(0, PEERS // 4 // peers)
    def _(step):
        start = pl.multiple_of(step * rows, rows)
        part = [parts[residue, pl.ds(start, rows), :] for residue in range(4)]
        even, odd = part[0] + part[2], part[1] + part[3]
        even_less, odd_less = part[0] - part[2], turned(part[1] - part[3])
        from_top = (lane_index(8) % 64 == WAVES) & packs_top
        for quarter, grid in enumerate([even + odd, even_less - odd_less, even - odd, even_less + odd_less]):
            for k in range(peers):
                fixed = {}
                for r in range(PITCH // 8):
                    tile = grid[k * PITCH + 8 * r : k * PITCH + 8 * r + 8]
                    fixed[r] = jnp.where(from_top, pltpu.roll(tile, 128 - WAVES, 1), tile)
                for tile, values in enumerate(packed(lambda slab, r: (fixed[r], 64 * slab))):
                    out_ref[quarter * (PEERS // 4) + step * peers + k, 8 * tile : 8 * tile + 8, :] = values


def share_kernel(in_ref, share_ref, everyone_ref, out_ref):
    lane = lane_index(1)
    levels = jnp.sum(everyone_ref[...], axis=0, keepdims=True)
    row = pltpu.roll(jnp.where(lane == 2, levels, share_ref[0:1, :]), SHARE_LANE, 1)
    shared = (lane >= SHARE_LANE) & (lane < SHARE_LANE + 3)
    tile = SHARE_ROW // 8 * 8
    here = lax.broadcasted_iota(jnp.int32, (8, 128), 0) == SHARE_ROW - tile
    for peer in range(PEERS):
        for start in range(0, 24, 8):
            values = in_ref[peer, start : start + 8, :]
            if start == tile:
                values = jnp.where(here & shared, row, values)
            out_ref[peer, start : start + 8, :] = values


def back_kernel(in_ref, table_ref, out_ref, energy_ref, total_ref):
    total = in_ref[0, SHARE_ROW : SHARE_ROW + 1, :]
    for peer in range(1, PEERS):
        total = total + in_ref[peer, SHARE_ROW : SHARE_ROW + 1, :]
    lane = lane_index(1) - SHARE_LANE
    energy_ref[0] = jnp.sum(jnp.where(lane == 0, total, 0.0))
    energy_ref[1] = jnp.sum(jnp.where(lane == 1, total, 0.0))
    total_ref[0] = jnp.sum(jnp.where(lane == 2, total, 0.0)) / (2 * lax.axis_size("lev"))
    parts = []
    for parity in range(2):
        rows = []
        for slab in range(2):
            for r in range(PITCH // 8):
                columns = []
                for v in range(COLUMNS // 128):
                    pieces = []
                    for place in range(v * GROUP, min((v + 1) * GROUP, SIDE)):
                        read = lambda tile: in_ref[parity * SIDE + place, 8 * tile : 8 * tile + 8, :]
                        pieces += pieces_of(read, slab, r, place % GROUP * WIDTH)
                    columns.append(gather_lanes(pieces))
                rows.append(jnp.concatenate(columns, axis=1))
        high, low = halves(jnp.concatenate(rows, axis=0))
        main = dot(jnp.concatenate([high, low], axis=0), table_ref[parity, 0])
        parts.append(main[:PAIR] + main[PAIR:] + dot(high, table_ref[parity, 1]))
    lower, upper = parts[0] + parts[1], parts[0] - parts[1]
    for slab in range(2):
        rows = slice(slab * PITCH, slab * PITCH + ROWS)
        out_ref[:, slab, :HALF] = lower[rows]
        out_ref[:, slab, HALF:] = upper[rows]


def grant(mebibytes):
    return pltpu.CompilerParams(vmem_limit_bytes=mebibytes << 20)


def in_hbm(array):
    return pltpu.with_memory_space_constraint(array, pltpu.HBM)


VMEM = pl.BlockSpec(memory_space=pltpu.VMEM)
HBM = pl.BlockSpec(memory_space=pltpu.HBM)
SMEM = pl.BlockSpec(memory_space=pltpu.SMEM)


def local(grid_field, truncation_limit, diffusion_order, diffusion_strength, mass_weight):
    row_forward, row_back = row_tables()
    column_forward, column_back = column_tables()
    block = jax.ShapeDtypeStruct((PEERS, 24, 128), jnp.float32)
    levels = lax.axis_size("lev")
    row_steps = 2 * COLUMNS // 256
    sent, lanes, damp = pl.pallas_call(
        row_kernel,
        out_shape=(
            block,
            jax.ShapeDtypeStruct((8, 128), jnp.float32),
            jax.ShapeDtypeStruct((4, QUARTER, 128), jnp.float32),
        ),
        in_specs=[HBM] * 6,
        out_specs=(VMEM, VMEM, VMEM),
        scratch_shapes=[
            pltpu.SMEM((N,), jnp.int32),
            pltpu.SMEM((2,), jnp.int32),
            pltpu.SMEM((2,), jnp.float32),
            pltpu.SMEM((2,), jnp.float32),
            pltpu.VMEM((ROWS, 2, N), jnp.float32),
            pltpu.VMEM((PAIR, 1280), jnp.float32),
            pltpu.VMEM((2, 2 * PAIR, HALF), jnp.bfloat16),
            pltpu.VMEM((row_steps, 2, HALF, 256), jnp.bfloat16),
            pltpu.SemaphoreType.DMA((row_steps + 1,)),
            pltpu.SemaphoreType.DMA((4,)),
        ],
        compiler_params=grant(14),
        name="row_forward",
    )(
        in_hbm(grid_field.transpose(1, 0, 2)),
        in_hbm(jnp.asarray(row_forward)),
        in_hbm(truncation_limit),
        in_hbm(diffusion_order),
        in_hbm(diffusion_strength),
        in_hbm(mass_weight),
    )
    received = lax.all_to_all(sent, "wav", split_axis=0, concat_axis=0, tiled=True)
    damped, share = pl.pallas_call(
        column_kernel,
        out_shape=(
            jax.ShapeDtypeStruct((4, QUARTER, 128), jnp.float32),
            jax.ShapeDtypeStruct((levels, 128), jnp.float32),
        ),
        in_specs=[VMEM] * 4,
        out_specs=(VMEM, VMEM),
        compiler_params=grant(10),
        name="column_forward",
    )(received, damp, lanes, jnp.asarray(column_forward))
    everyone = lax.all_to_all(share, "lev", split_axis=0, concat_axis=0, tiled=True)
    column_back_call = pl.pallas_call(
        column_back_kernel,
        out_shape=block,
        in_specs=[VMEM, VMEM, HBM],
        out_specs=VMEM,
        scratch_shapes=[
            pltpu.VMEM(column_back.shape, jnp.bfloat16),
            pltpu.VMEM((4, BLOCK, 128), jnp.float32),
            pltpu.SemaphoreType.DMA((4,)),
        ],
        compiler_params=grant(10),
        cost_estimate=pl.CostEstimate(flops=2_000_000_000, bytes_accessed=6_000_000, transcendentals=0),
        name="column_back",
    )
    back = column_back_call(damped, lanes, in_hbm(jnp.asarray(column_back)))
    back = pl.pallas_call(
        share_kernel,
        out_shape=block,
        in_specs=[VMEM] * 3,
        out_specs=VMEM,
        compiler_params=grant(2),
        cost_estimate=pl.CostEstimate(flops=4_000_000_000, bytes_accessed=800_000, transcendentals=0),
        name="share",
    )(back, share, everyone)
    returned = lax.all_to_all(back, "wav", split_axis=0, concat_axis=0, tiled=True)
    filtered, energies, total_energy = pl.pallas_call(
        back_kernel,
        out_shape=(
            jax.ShapeDtypeStruct((ROWS, 2, N), jnp.float32),
            jax.ShapeDtypeStruct((2,), jnp.float32),
            jax.ShapeDtypeStruct((1,), jnp.float32),
        ),
        in_specs=[VMEM, VMEM],
        out_specs=(VMEM, SMEM, SMEM),
        compiler_params=grant(10),
        name="row_back",
    )(returned, jnp.asarray(row_back))
    return filtered.transpose(1, 0, 2), energies, total_energy.reshape(())


def solution(mesh):
    placed = (P("lev", "wav", None), P(), P("lev"), P("lev"), P("lev"))
    return jax.shard_map(
        local,
        mesh=mesh,
        in_specs=placed,
        out_specs=(P("lev", "wav", None), P("lev"), P()),
        check_vma=False,
    )
```

```python
import functools
import math

import jax
import jax.numpy as jnp
import ml_dtypes
import numpy as np
from jax import lax
from jax.experimental import pallas as pl
from jax.experimental.pallas import tpu as pltpu
from jax.sharding import PartitionSpec as P

N = 1216
HALF = N // 2
QUARTER = N // 4
PEERS = 32
ROWS = N // PEERS
PITCH = 40
WAVES = HALF // PEERS
WIDTH = 2 * WAVES
SIDE = PEERS // 2
GROUP = 3
COLUMNS = -(-SIDE // GROUP) * 128
BLOCK = PEERS // 4 * PITCH
PAIR = 2 * PITCH
SLOTS = {
    (0, 0): [(0, 0, 0, WIDTH)],
    (0, 1): [(1, 0, 0, WIDTH)],
    (0, 2): [(2, 0, 0, WIDTH)],
    (1, 0): [(0, 38, 0, WIDTH)],
    (1, 1): [(1, 38, 0, WIDTH)],
    (1, 2): [(2, 38, 0, WIDTH)],
    (0, 3): [(0, 76, 0, WIDTH)],
    (1, 3): [(1, 76, 0, WIDTH)],
    (0, 4): [(2, 76, 0, WIDTH)],
    (1, 4): [(0, 114, 0, 14), (1, 114, 14, 14), (2, 114, 28, 10)],
}

SHARE_ROW, SHARE_LANE = 16 + ROWS - 32, 76


def split(table):
    high = table.astype(ml_dtypes.bfloat16)
    low = (table - high.astype(np.float64)).astype(ml_dtypes.bfloat16)
    return high, low


def angle(product):
    return (product % N).astype(np.float64) * (2.0 * math.pi / N)


@functools.cache
def row_tables():
    j = np.arange(HALF)
    forward = np.zeros((2, HALF, COLUMNS))
    back = np.zeros((2, COLUMNS, HALF))
    for parity in range(2):
        for place in range(SIDE):
            wave = 2 * (place * WAVES + np.arange(WAVES)) + parity
            theta = angle(j[:, None] * wave[None, :])
            cosine, sine = np.cos(theta), -np.sin(theta)
            weight = np.where(wave == 0, 1.0, 2.0)
            if wave[0] == 0:
                sine[:, 0] = np.cos(angle(j * HALF))
            both = np.concatenate([cosine, sine], axis=1)
            start = place // GROUP * 128 + place % GROUP * WIDTH
            forward[parity, :, start : start + WIDTH] = both
            back[parity, start : start + WIDTH, :] = (
                both * np.concatenate([weight, weight]) / float(N) ** 2
            ).T
    return (
        np.stack([np.stack(split(t)) for t in forward]),
        np.stack([np.stack(split(t)) for t in back]),
    )


@functools.cache
def column_tables():
    place = np.full((PEERS // 4, PITCH), -1, np.int64)
    place[:, :ROWS] = np.arange(QUARTER).reshape(PEERS // 4, ROWS)
    place = place.reshape(-1)
    used = (place >= 0).astype(np.float64)
    spot = np.maximum(place, 0)
    m = np.arange(QUARTER)
    forward, back = [], []
    for residue in range(4):
        theta = angle((4 * m + residue)[:, None] * spot[None, :])
        cosine, sine = np.cos(theta) * used, np.sin(theta) * used
        forward.append(np.concatenate(split(np.concatenate([cosine, sine], axis=1)), axis=0))
        back.append(np.concatenate(split(np.concatenate([cosine.T, -sine.T], axis=1)), axis=0))
    return np.stack(forward), np.stack(back)


def dot(left, right):
    return lax.dot_general(left, right, (((1,), (0,)), ((), ())), preferred_element_type=jnp.float32)


def halves(values):
    high = values.astype(jnp.bfloat16)
    low = (values - high.astype(jnp.float32)).astype(jnp.bfloat16)
    return high, low


def lane_index(rows):
    return lax.broadcasted_iota(jnp.int32, (rows, 128), 1)


def turn(values, shift):
    return values if shift % 128 == 0 else pltpu.roll(values, shift % 128, 1)


def gather_lanes(pieces):
    lane = lane_index(8)
    result = None
    for values, source, target in pieces:
        turned = turn(values, target - source)
        result = turned if result is None else jnp.where(lane >= target, turned, result)
    return result


def packed(read):
    tiles = []
    for tile in range(3):
        pieces = []
        for (slab, r), slots in SLOTS.items():
            for where, lane, first, _ in slots:
                if where == tile:
                    values, start = read(slab, r)
                    pieces.append((values, start + first, lane))
        tiles.append(gather_lanes(sorted(pieces, key=lambda p: p[2])))
    return tiles


def pieces_of(read, slab, r, target):
    return [(read(tile), lane, target + first) for tile, lane, first, _ in SLOTS[slab, r]]


def row_kernel(
    grid_ref, table_ref, limit_in, order_in, strength_in, mass_in, out_ref, lane_ref, damp_ref,
    limit_ref, order_ref, strength_ref, mass_ref, x_ref, xs, both, held, sem, small_sem,
):
    chunk = 256
    count = COLUMNS // chunk
    inside = chunk // 128 * GROUP

    def table_copy(step):
        columns = pl.ds(pl.multiple_of(step % count * chunk, chunk), chunk)
        return pltpu.make_async_copy(
            table_ref.at[step // count, :, :, columns], held.at[step], sem.at[step]
        )

    small_copies = [
        pltpu.make_async_copy(source, target, small_sem.at[k])
        for k, (source, target) in enumerate(
            [(limit_in, limit_ref), (order_in, order_ref), (strength_in, strength_ref), (mass_in, mass_ref)]
        )
    ]
    for copy in small_copies:
        copy.start()
    grid_copy = pltpu.make_async_copy(grid_ref, x_ref, sem.at[2 * count])
    grid_copy.start()
    for step in range(2 * count):
        table_copy(step).start()
    lane_ref[...] = jnp.zeros_like(lane_ref)
    for copy in small_copies:
        copy.wait()
    fill_lanes(lane_ref, limit_ref, order_ref, strength_ref, mass_ref)
    fill_damping(lane_ref, damp_ref)
    xs[...] = jnp.zeros_like(xs)
    grid_copy.wait()
    for slab in range(2):
        xs[slab * PITCH : slab * PITCH + ROWS, :N] = x_ref[:, slab, :]
    full = xs[...]
    turned = pltpu.roll(full, full.shape[1] - HALF, 1)
    for parity in range(2):
        value = (full + turned if parity == 0 else full - turned)[:, :HALF]
        high, low = halves(value)
        both[parity, :PAIR] = high
        both[parity, PAIR:] = low

    for step in range(2 * count):
        table_copy(step).wait()
    for step in range(2 * count):
        parity, k = step // count, step % count
        main = dot(both[parity], held[step, 0])
        result = main[:PAIR] + main[PAIR:] + dot(both[parity, :PAIR], held[step, 1])
        for spot in range(min(inside, SIDE - k * inside)):
            start = spot // GROUP * 128

            def read(slab, r):
                rows = slice(slab * PITCH + 8 * r, slab * PITCH + 8 * r + 8)
                return result[rows, start : start + 128], spot % GROUP * WIDTH

            for tile, values in enumerate(packed(read)):
                out_ref[parity * SIDE + k * inside + spot, 8 * tile : 8 * tile + 8, :] = values


def fill_lanes(lane_ref, limit_ref, order_ref, strength_ref, mass_ref):
    place = lax.axis_index("wav")
    parity, spot = place // SIDE, place % SIDE
    lane = lane_index(1)
    column = lane % 64
    slot = jnp.where(column < WAVES, column, column - WAVES)
    regular = column < WIDTH
    wave = jnp.where(regular, 2 * (spot * WAVES + slot) + parity, HALF)
    limit = jnp.broadcast_to(limit_ref[HALF], (1, 128))
    for k in range(WAVES):
        limit = jnp.where(regular & (slot == k), limit_ref[2 * (spot * WAVES + k) + parity], limit)
    weight = jnp.where((wave == 0) | (wave == HALF), 1.0, 2.0) / float(N) ** 4
    top = ((column == WIDTH) | (column == WIDTH + WAVES)) & (place == 0)
    first = lane < 64
    wave = wave.astype(jnp.float32)
    rows = [
        wave * wave,
        limit.astype(jnp.float32),
        jnp.where(first, order_ref[0], order_ref[1]).astype(jnp.float32),
        jnp.where(first, strength_ref[0], strength_ref[1]),
        jnp.where(regular | top, weight, 0.0),
        jnp.where(jnp.broadcast_to(place, (1, 128)) == 0, 1.0, 0.0),
        jnp.where(first, mass_ref[0], mass_ref[1]),
    ]
    for k, row in enumerate(rows):
        lane_ref[k : k + 1, :] = row


def fill_damping(lane_ref, damp_ref):
    wave_square = lane_ref[0:1, :]
    limit = lane_ref[1:2, :]
    order = lane_ref[2:3, :]
    strength = lane_ref[3:4, :]

    @pl.loop(0, 4)
    def _(residue):
        q = 4 * lax.broadcasted_iota(jnp.int32, (QUARTER, 128), 0) + residue
        wave = jnp.where(q < HALF, q, q - N).astype(jnp.float32)
        radius = (wave_square + wave * wave) / (0.5 * N) ** 2
        square = radius * radius
        powered = jnp.where(
            order == 1.0,
            radius,
            jnp.where(order == 2.0, square, jnp.where(order == 3.0, square * radius, square * square)),
        )
        damp_ref[residue] = jnp.where(jnp.abs(wave) <= limit, 1.0 / (1.0 + strength * powered), 0.0)


def turned(values):
    forward = pltpu.roll(values, 128 - WAVES, 1)
    backward = pltpu.roll(values, WAVES, 1)
    spot = lane_index(values.shape[0]) % 64
    return jnp.where((spot < WAVES) | (spot == WIDTH), forward, -backward)


def folded(result):
    count = result.shape[0] // 2
    both = result[:count] + result[count:]
    return both[:, :128] + both[:, 128:]


def weights(values, other):
    return jnp.concatenate(
        [jnp.concatenate(halves(values), axis=1), jnp.concatenate(halves(other), axis=1)], axis=0
    )


def column_kernel(in_ref, damp_ref, lane_ref, table_ref, out_ref, share_ref):
    packs_top = lane_ref[5:6, :] > 0.5
    spot = lane_index(8) % 64
    to_top = (spot == WIDTH) & packs_top
    cleared = ((spot == WAVES) | (spot == WIDTH + WAVES)) & packs_top
    quarters = []
    for quarter in range(4):
        tiles = []
        for peer in range(quarter * PEERS // 4, (quarter + 1) * PEERS // 4):
            read = lambda tile: in_ref[peer, 8 * tile : 8 * tile + 8, :]
            for r in range(PITCH // 8):
                tile = gather_lanes(pieces_of(read, 0, r, 0) + pieces_of(read, 1, r, 64))
                tile = jnp.where(to_top, pltpu.roll(tile, WAVES, 1), jnp.where(cleared, 0.0, tile))
                tiles.append(tile)
        quarters.append(jnp.concatenate(tiles, axis=0))
    c, d = quarters[0] + quarters[2], quarters[1] + quarters[3]
    a, b = quarters[0] - quarters[2], quarters[1] - quarters[3]
    turned_c, turned_d, turned_a, turned_b = turned(c), turned(d), turned(a), turned(b)
    inputs = [
        (c + d, turned_c + turned_d),
        (a + turned_b, turned_a - b),
        (c - d, turned_c - turned_d),
        (a - turned_b, turned_a + b),
    ]
    energy = jnp.zeros((8, 128), jnp.float32)
    for residue in range(4):
        damped = folded(dot(table_ref[residue], weights(*inputs[residue]))) * damp_ref[residue]
        out_ref[residue] = damped
        energy = energy + jnp.sum((damped * damped).reshape(QUARTER // 8, 8, 128), axis=0)
    energy = jnp.sum(energy, axis=0, keepdims=True) * lane_ref[4:5, :]
    lane = lane_index(1)
    first = jnp.sum(jnp.where(lane < 64, energy, 0.0), axis=1, keepdims=True)
    second = jnp.sum(jnp.where(lane < 64, 0.0, energy), axis=1, keepdims=True)
    weighted = jnp.sum(energy * lane_ref[6:7, :], axis=1, keepdims=True)
    row = jnp.where(lane == 0, first, jnp.where(lane == 1, second, jnp.where(lane == 2, weighted, 0.0)))
    share_ref[...] = jnp.broadcast_to(row, share_ref.shape)


def column_back_kernel(in_ref, lane_ref, table_ref, out_ref, held, parts, sem):
    def table_copy(residue):
        return pltpu.make_async_copy(table_ref.at[residue], held.at[residue], sem.at[residue])

    for residue in range(4):
        table_copy(residue).start()
    packs_top = lane_ref[5:6, :] > 0.5
    peers = 2
    rows = peers * PITCH

    @pl.loop(0, 4)
    def _(residue):
        damped = in_ref[residue]
        table_copy(residue).wait()
        parts[residue] = folded(dot(held[residue], weights(damped, turned(damped))))

    @pl.loop(0, PEERS // 4 // peers)
    def _(step):
        start = pl.multiple_of(step * rows, rows)
        part = [parts[residue, pl.ds(start, rows), :] for residue in range(4)]
        even, odd = part[0] + part[2], part[1] + part[3]
        even_less, odd_less = part[0] - part[2], turned(part[1] - part[3])
        from_top = (lane_index(8) % 64 == WAVES) & packs_top
        for quarter, grid in enumerate([even + odd, even_less - odd_less, even - odd, even_less + odd_less]):
            for k in range(peers):
                fixed = {}
                for r in range(PITCH // 8):
                    tile = grid[k * PITCH + 8 * r : k * PITCH + 8 * r + 8]
                    fixed[r] = jnp.where(from_top, pltpu.roll(tile, 128 - WAVES, 1), tile)
                for tile, values in enumerate(packed(lambda slab, r: (fixed[r], 64 * slab))):
                    out_ref[quarter * (PEERS // 4) + step * peers + k, 8 * tile : 8 * tile + 8, :] = values


def share_kernel(in_ref, share_ref, everyone_ref, out_ref):
    lane = lane_index(1)
    levels = jnp.sum(everyone_ref[...], axis=0, keepdims=True)
    row = pltpu.roll(jnp.where(lane == 2, levels, share_ref[0:1, :]), SHARE_LANE, 1)
    shared = (lane >= SHARE_LANE) & (lane < SHARE_LANE + 3)
    tile = SHARE_ROW // 8 * 8
    here = lax.broadcasted_iota(jnp.int32, (8, 128), 0) == SHARE_ROW - tile
    for peer in range(PEERS):
        for start in range(0, 24, 8):
            values = in_ref[peer, start : start + 8, :]
            if start == tile:
                values = jnp.where(here & shared, row, values)
            out_ref[peer, start : start + 8, :] = values


def back_kernel(in_ref, table_ref, out_ref, energy_ref, total_ref):
    total = in_ref[0, SHARE_ROW : SHARE_ROW + 1, :]
    for peer in range(1, PEERS):
        total = total + in_ref[peer, SHARE_ROW : SHARE_ROW + 1, :]
    lane = lane_index(1) - SHARE_LANE
    energy_ref[0] = jnp.sum(jnp.where(lane == 0, total, 0.0))
    energy_ref[1] = jnp.sum(jnp.where(lane == 1, total, 0.0))
    total_ref[0] = jnp.sum(jnp.where(lane == 2, total, 0.0)) / (2 * lax.axis_size("lev"))
    parts = []
    for parity in range(2):
        rows = []
        for slab in range(2):
            for r in range(PITCH // 8):
                columns = []
                for v in range(COLUMNS // 128):
                    pieces = []
                    for place in range(v * GROUP, min((v + 1) * GROUP, SIDE)):
                        read = lambda tile: in_ref[parity * SIDE + place, 8 * tile : 8 * tile + 8, :]
                        pieces += pieces_of(read, slab, r, place % GROUP * WIDTH)
                    columns.append(gather_lanes(pieces))
                rows.append(jnp.concatenate(columns, axis=1))
        high, low = halves(jnp.concatenate(rows, axis=0))
        main = dot(jnp.concatenate([high, low], axis=0), table_ref[parity, 0])
        parts.append(main[:PAIR] + main[PAIR:] + dot(high, table_ref[parity, 1]))
    lower, upper = parts[0] + parts[1], parts[0] - parts[1]
    for slab in range(2):
        rows = slice(slab * PITCH, slab * PITCH + ROWS)
        out_ref[:, slab, :HALF] = lower[rows]
        out_ref[:, slab, HALF:] = upper[rows]


def grant(mebibytes):
    return pltpu.CompilerParams(vmem_limit_bytes=mebibytes << 20)


def in_hbm(array):
    return pltpu.with_memory_space_constraint(array, pltpu.HBM)


VMEM = pl.BlockSpec(memory_space=pltpu.VMEM)
HBM = pl.BlockSpec(memory_space=pltpu.HBM)
SMEM = pl.BlockSpec(memory_space=pltpu.SMEM)


def local(grid_field, truncation_limit, diffusion_order, diffusion_strength, mass_weight):
    row_forward, row_back = row_tables()
    column_forward, column_back = column_tables()
    block = jax.ShapeDtypeStruct((PEERS, 24, 128), jnp.float32)
    levels = lax.axis_size("lev")
    row_steps = 2 * COLUMNS // 256
    sent, lanes, damp = pl.pallas_call(
        row_kernel,
        out_shape=(
            block,
            jax.ShapeDtypeStruct((8, 128), jnp.float32),
            jax.ShapeDtypeStruct((4, QUARTER, 128), jnp.float32),
        ),
        in_specs=[HBM] * 6,
        out_specs=(VMEM, VMEM, VMEM),
        scratch_shapes=[
            pltpu.SMEM((N,), jnp.int32),
            pltpu.SMEM((2,), jnp.int32),
            pltpu.SMEM((2,), jnp.float32),
            pltpu.SMEM((2,), jnp.float32),
            pltpu.VMEM((ROWS, 2, N), jnp.float32),
            pltpu.VMEM((PAIR, 1280), jnp.float32),
            pltpu.VMEM((2, 2 * PAIR, HALF), jnp.bfloat16),
            pltpu.VMEM((row_steps, 2, HALF, 256), jnp.bfloat16),
            pltpu.SemaphoreType.DMA((row_steps + 1,)),
            pltpu.SemaphoreType.DMA((4,)),
        ],
        compiler_params=grant(14),
        name="row_forward",
    )(
        in_hbm(grid_field.transpose(1, 0, 2)),
        in_hbm(jnp.asarray(row_forward)),
        in_hbm(truncation_limit),
        in_hbm(diffusion_order),
        in_hbm(diffusion_strength),
        in_hbm(mass_weight),
    )
    received = lax.all_to_all(sent, "wav", split_axis=0, concat_axis=0, tiled=True)
    damped, share = pl.pallas_call(
        column_kernel,
        out_shape=(
            jax.ShapeDtypeStruct((4, QUARTER, 128), jnp.float32),
            jax.ShapeDtypeStruct((levels, 128), jnp.float32),
        ),
        in_specs=[VMEM] * 4,
        out_specs=(VMEM, VMEM),
        compiler_params=grant(10),
        name="column_forward",
    )(received, damp, lanes, jnp.asarray(column_forward))
    everyone = lax.all_to_all(share, "lev", split_axis=0, concat_axis=0, tiled=True)
    column_back_call = pl.pallas_call(
        column_back_kernel,
        out_shape=block,
        in_specs=[VMEM, VMEM, HBM],
        out_specs=VMEM,
        scratch_shapes=[
            pltpu.VMEM(column_back.shape, jnp.bfloat16),
            pltpu.VMEM((4, BLOCK, 128), jnp.float32),
            pltpu.SemaphoreType.DMA((4,)),
        ],
        compiler_params=grant(10),
        cost_estimate=pl.CostEstimate(flops=2_000_000_000, bytes_accessed=6_000_000, transcendentals=0),
        name="column_back",
    )
    back = column_back_call(damped, lanes, in_hbm(jnp.asarray(column_back)))
    back = pl.pallas_call(
        share_kernel,
        out_shape=block,
        in_specs=[VMEM] * 3,
        out_specs=VMEM,
        compiler_params=grant(2),
        cost_estimate=pl.CostEstimate(flops=4_000_000_000, bytes_accessed=800_000, transcendentals=0),
        name="share",
    )(back, share, everyone)
    returned = lax.all_to_all(back, "wav", split_axis=0, concat_axis=0, tiled=True)
    filtered, energies, total_energy = pl.pallas_call(
        back_kernel,
        out_shape=(
            jax.ShapeDtypeStruct((ROWS, 2, N), jnp.float32),
            jax.ShapeDtypeStruct((2,), jnp.float32),
            jax.ShapeDtypeStruct((1,), jnp.float32),
        ),
        in_specs=[VMEM, VMEM],
        out_specs=(VMEM, SMEM, SMEM),
        compiler_params=grant(10),
        name="row_back",
    )(returned, jnp.asarray(row_back))
    return filtered.transpose(1, 0, 2), energies, total_energy.reshape(())


def solution(mesh):
    placed = (P("lev", "wav", None), P(), P("lev"), P("lev"), P("lev"))
    return jax.shard_map(
        local,
        mesh=mesh,
        in_specs=placed,
        out_specs=(P("lev", "wav", None), P("lev"), P()),
        check_vma=False,
    )
```

```python
import functools
import math

import jax
import jax.numpy as jnp
import ml_dtypes
import numpy as np
from jax import lax
from jax.experimental import pallas as pl
from jax.experimental.pallas import tpu as pltpu
from jax.sharding import PartitionSpec as P

N = 1216
HALF = N // 2
QUARTER = N // 4
PEERS = 32
ROWS = N // PEERS
PITCH = 40
WAVES = HALF // PEERS
WIDTH = 2 * WAVES
SIDE = PEERS // 2
GROUP = 3
COLUMNS = -(-SIDE // GROUP) * 128
BLOCK = PEERS // 4 * PITCH
PAIR = 2 * PITCH
SLOTS = {
    (0, 0): [(0, 0, 0, WIDTH)],
    (0, 1): [(1, 0, 0, WIDTH)],
    (0, 2): [(2, 0, 0, WIDTH)],
    (1, 0): [(0, 38, 0, WIDTH)],
    (1, 1): [(1, 38, 0, WIDTH)],
    (1, 2): [(2, 38, 0, WIDTH)],
    (0, 3): [(0, 76, 0, WIDTH)],
    (1, 3): [(1, 76, 0, WIDTH)],
    (0, 4): [(2, 76, 0, WIDTH)],
    (1, 4): [(0, 114, 0, 14), (1, 114, 14, 14), (2, 114, 28, 10)],
}

SHARE_ROW, SHARE_LANE = 16 + ROWS - 32, 76


def split(table):
    high = table.astype(ml_dtypes.bfloat16)
    low = (table - high.astype(np.float64)).astype(ml_dtypes.bfloat16)
    return high, low


def angle(product):
    return (product % N).astype(np.float64) * (2.0 * math.pi / N)


@functools.cache
def row_tables():
    j = np.arange(HALF)
    forward = np.zeros((2, HALF, COLUMNS))
    back = np.zeros((2, COLUMNS, HALF))
    for parity in range(2):
        for place in range(SIDE):
            wave = 2 * (place * WAVES + np.arange(WAVES)) + parity
            theta = angle(j[:, None] * wave[None, :])
            cosine, sine = np.cos(theta), -np.sin(theta)
            weight = np.where(wave == 0, 1.0, 2.0)
            if wave[0] == 0:
                sine[:, 0] = np.cos(angle(j * HALF))
            both = np.concatenate([cosine, sine], axis=1)
            start = place // GROUP * 128 + place % GROUP * WIDTH
            forward[parity, :, start : start + WIDTH] = both
            back[parity, start : start + WIDTH, :] = (
                both * np.concatenate([weight, weight]) / float(N) ** 2
            ).T
    return (
        np.stack([np.stack(split(t)) for t in forward]),
        np.stack([np.stack(split(t)) for t in back]),
    )


@functools.cache
def column_tables():
    place = np.full((PEERS // 4, PITCH), -1, np.int64)
    place[:, :ROWS] = np.arange(QUARTER).reshape(PEERS // 4, ROWS)
    place = place.reshape(-1)
    used = (place >= 0).astype(np.float64)
    spot = np.maximum(place, 0)
    m = np.arange(QUARTER)
    forward, back = [], []
    for residue in range(4):
        theta = angle((4 * m + residue)[:, None] * spot[None, :])
        cosine, sine = np.cos(theta) * used, np.sin(theta) * used
        forward.append(np.concatenate(split(np.concatenate([cosine, sine], axis=1)), axis=0))
        back.append(np.concatenate(split(np.concatenate([cosine.T, -sine.T], axis=1)), axis=0))
    return np.stack(forward), np.stack(back)


def dot(left, right):
    return lax.dot_general(left, right, (((1,), (0,)), ((), ())), preferred_element_type=jnp.float32)


def halves(values):
    high = values.astype(jnp.bfloat16)
    low = (values - high.astype(jnp.float32)).astype(jnp.bfloat16)
    return high, low


def lane_index(rows):
    return lax.broadcasted_iota(jnp.int32, (rows, 128), 1)


def turn(values, shift):
    return values if shift % 128 == 0 else pltpu.roll(values, shift % 128, 1)


def gather_lanes(pieces):
    lane = lane_index(8)
    result = None
    for values, source, target in pieces:
        turned = turn(values, target - source)
        result = turned if result is None else jnp.where(lane >= target, turned, result)
    return result


def packed(read):
    tiles = []
    for tile in range(3):
        pieces = []
        for (slab, r), slots in SLOTS.items():
            for where, lane, first, _ in slots:
                if where == tile:
                    values, start = read(slab, r)
                    pieces.append((values, start + first, lane))
        tiles.append(gather_lanes(sorted(pieces, key=lambda p: p[2])))
    return tiles


def pieces_of(read, slab, r, target):
    return [(read(tile), lane, target + first) for tile, lane, first, _ in SLOTS[slab, r]]


def row_kernel(
    grid_ref, table_ref, limit_in, order_in, strength_in, mass_in, out_ref, lane_ref, damp_ref,
    limit_ref, order_ref, strength_ref, mass_ref, x_ref, xs, both, held, sem, small_sem,
):
    chunk = 256
    count = COLUMNS // chunk
    inside = chunk // 128 * GROUP

    def table_copy(step):
        columns = pl.ds(pl.multiple_of(step % count * chunk, chunk), chunk)
        return pltpu.make_async_copy(
            table_ref.at[step // count, :, :, columns], held.at[step], sem.at[step]
        )

    small_copies = [
        pltpu.make_async_copy(source, target, small_sem.at[k])
        for k, (source, target) in enumerate(
            [(limit_in, limit_ref), (order_in, order_ref), (strength_in, strength_ref), (mass_in, mass_ref)]
        )
    ]
    for copy in small_copies:
        copy.start()
    grid_copy = pltpu.make_async_copy(grid_ref, x_ref, sem.at[2 * count])
    grid_copy.start()
    for step in range(2 * count):
        table_copy(step).start()
    lane_ref[...] = jnp.zeros_like(lane_ref)
    for copy in small_copies:
        copy.wait()
    fill_lanes(lane_ref, limit_ref, order_ref, strength_ref, mass_ref)
    fill_damping(lane_ref, damp_ref)
    xs[...] = jnp.zeros_like(xs)
    grid_copy.wait()
    for slab in range(2):
        xs[slab * PITCH : slab * PITCH + ROWS, :N] = x_ref[:, slab, :]
    full = xs[...]
    turned = pltpu.roll(full, full.shape[1] - HALF, 1)
    for parity in range(2):
        value = (full + turned if parity == 0 else full - turned)[:, :HALF]
        high, low = halves(value)
        both[parity, :PAIR] = high
        both[parity, PAIR:] = low

    for step in range(2 * count):
        table_copy(step).wait()
    for step in range(2 * count):
        parity, k = step // count, step % count
        main = dot(both[parity], held[step, 0])
        result = main[:PAIR] + main[PAIR:] + dot(both[parity, :PAIR], held[step, 1])
        for spot in range(min(inside, SIDE - k * inside)):
            start = spot // GROUP * 128

            def read(slab, r):
                rows = slice(slab * PITCH + 8 * r, slab * PITCH + 8 * r + 8)
                return result[rows, start : start + 128], spot % GROUP * WIDTH

            for tile, values in enumerate(packed(read)):
                out_ref[parity * SIDE + k * inside + spot, 8 * tile : 8 * tile + 8, :] = values


def fill_lanes(lane_ref, limit_ref, order_ref, strength_ref, mass_ref):
    place = lax.axis_index("wav")
    parity, spot = place // SIDE, place % SIDE
    lane = lane_index(1)
    column = lane % 64
    slot = jnp.where(column < WAVES, column, column - WAVES)
    regular = column < WIDTH
    wave = jnp.where(regular, 2 * (spot * WAVES + slot) + parity, HALF)
    limit = jnp.broadcast_to(limit_ref[HALF], (1, 128))
    for k in range(WAVES):
        limit = jnp.where(regular & (slot == k), limit_ref[2 * (spot * WAVES + k) + parity], limit)
    weight = jnp.where((wave == 0) | (wave == HALF), 1.0, 2.0) / float(N) ** 4
    top = ((column == WIDTH) | (column == WIDTH + WAVES)) & (place == 0)
    first = lane < 64
    wave = wave.astype(jnp.float32)
    rows = [
        wave * wave,
        limit.astype(jnp.float32),
        jnp.where(first, order_ref[0], order_ref[1]).astype(jnp.float32),
        jnp.where(first, strength_ref[0], strength_ref[1]),
        jnp.where(regular | top, weight, 0.0),
        jnp.where(jnp.broadcast_to(place, (1, 128)) == 0, 1.0, 0.0),
        jnp.where(first, mass_ref[0], mass_ref[1]),
    ]
    for k, row in enumerate(rows):
        lane_ref[k : k + 1, :] = row


def fill_damping(lane_ref, damp_ref):
    wave_square = lane_ref[0:1, :]
    limit = lane_ref[1:2, :]
    order = lane_ref[2:3, :]
    strength = lane_ref[3:4, :]

    @pl.loop(0, 4)
    def _(residue):
        q = 4 * lax.broadcasted_iota(jnp.int32, (QUARTER, 128), 0) + residue
        wave = jnp.where(q < HALF, q, q - N).astype(jnp.float32)
        radius = (wave_square + wave * wave) / (0.5 * N) ** 2
        square = radius * radius
        powered = jnp.where(
            order == 1.0,
            radius,
            jnp.where(order == 2.0, square, jnp.where(order == 3.0, square * radius, square * square)),
        )
        damp_ref[residue] = jnp.where(jnp.abs(wave) <= limit, 1.0 / (1.0 + strength * powered), 0.0)


def turned(values):
    forward = pltpu.roll(values, 128 - WAVES, 1)
    backward = pltpu.roll(values, WAVES, 1)
    spot = lane_index(values.shape[0]) % 64
    return jnp.where((spot < WAVES) | (spot == WIDTH), forward, -backward)


def folded(result):
    count = result.shape[0] // 2
    both = result[:count] + result[count:]
    return both[:, :128] + both[:, 128:]


def weights(values, other):
    return jnp.concatenate(
        [jnp.concatenate(halves(values), axis=1), jnp.concatenate(halves(other), axis=1)], axis=0
    )


def column_kernel(in_ref, damp_ref, lane_ref, table_ref, out_ref, share_ref, kept_ref):
    packs_top = lane_ref[5:6, :] > 0.5
    spot = lane_index(8) % 64
    to_top = (spot == WIDTH) & packs_top
    cleared = ((spot == WAVES) | (spot == WIDTH + WAVES)) & packs_top
    quarters = []
    for quarter in range(4):
        tiles = []
        for peer in range(quarter * PEERS // 4, (quarter + 1) * PEERS // 4):
            read = lambda tile: in_ref[peer, 8 * tile : 8 * tile + 8, :]
            for r in range(PITCH // 8):
                tile = gather_lanes(pieces_of(read, 0, r, 0) + pieces_of(read, 1, r, 64))
                tile = jnp.where(to_top, pltpu.roll(tile, WAVES, 1), jnp.where(cleared, 0.0, tile))
                tiles.append(tile)
        quarters.append(jnp.concatenate(tiles, axis=0))
    c, d = quarters[0] + quarters[2], quarters[1] + quarters[3]
    a, b = quarters[0] - quarters[2], quarters[1] - quarters[3]
    turned_c, turned_d, turned_a, turned_b = turned(c), turned(d), turned(a), turned(b)
    inputs = [
        (c + d, turned_c + turned_d),
        (a + turned_b, turned_a - b),
        (c - d, turned_c - turned_d),
        (a - turned_b, turned_a + b),
    ]
    energy = jnp.zeros((8, 128), jnp.float32)
    for residue in range(4):
        damped = folded(dot(table_ref[residue], weights(*inputs[residue]))) * damp_ref[residue]
        out_ref[residue] = damped
        energy = energy + jnp.sum((damped * damped).reshape(QUARTER // 8, 8, 128), axis=0)
    energy = jnp.sum(energy, axis=0, keepdims=True) * lane_ref[4:5, :]
    lane = lane_index(1)
    first = jnp.sum(jnp.where(lane < 64, energy, 0.0), axis=1, keepdims=True)
    second = jnp.sum(jnp.where(lane < 64, 0.0, energy), axis=1, keepdims=True)
    weighted = jnp.sum(energy * lane_ref[6:7, :], axis=1, keepdims=True)
    row = jnp.where(lane == 0, first, jnp.where(lane == 1, second, jnp.where(lane == 2, weighted, 0.0)))
    share_ref[...] = jnp.broadcast_to(row, share_ref.shape)
    kept_ref[...] = jnp.broadcast_to(row, kept_ref.shape)


def column_back_kernel(in_ref, lane_ref, table_ref, out_ref, held, parts, sem):
    def table_copy(residue):
        return pltpu.make_async_copy(table_ref.at[residue], held.at[residue], sem.at[residue])

    for residue in range(4):
        table_copy(residue).start()
    packs_top = lane_ref[5:6, :] > 0.5
    peers = 2
    rows = peers * PITCH

    @pl.loop(0, 4)
    def _(residue):
        damped = in_ref[residue]
        table_copy(residue).wait()
        parts[residue] = folded(dot(held[residue], weights(damped, turned(damped))))

    @pl.loop(0, PEERS // 4 // peers)
    def _(step):
        start = pl.multiple_of(step * rows, rows)
        part = [parts[residue, pl.ds(start, rows), :] for residue in range(4)]
        even, odd = part[0] + part[2], part[1] + part[3]
        even_less, odd_less = part[0] - part[2], turned(part[1] - part[3])
        from_top = (lane_index(8) % 64 == WAVES) & packs_top
        for quarter, grid in enumerate([even + odd, even_less - odd_less, even - odd, even_less + odd_less]):
            for k in range(peers):
                fixed = {}
                for r in range(PITCH // 8):
                    tile = grid[k * PITCH + 8 * r : k * PITCH + 8 * r + 8]
                    fixed[r] = jnp.where(from_top, pltpu.roll(tile, 128 - WAVES, 1), tile)
                for tile, values in enumerate(packed(lambda slab, r: (fixed[r], 64 * slab))):
                    out_ref[quarter * (PEERS // 4) + step * peers + k, 8 * tile : 8 * tile + 8, :] = values


def share_kernel(in_ref, share_ref, everyone_ref, out_ref):
    lane = lane_index(1)
    levels = jnp.sum(everyone_ref[...], axis=0, keepdims=True)
    row = pltpu.roll(jnp.where(lane == 2, levels, share_ref[0:1, :]), SHARE_LANE, 1)
    shared = (lane >= SHARE_LANE) & (lane < SHARE_LANE + 3)
    tile = SHARE_ROW // 8 * 8
    here = lax.broadcasted_iota(jnp.int32, (8, 128), 0) == SHARE_ROW - tile
    for peer in range(PEERS):
        for start in range(0, 24, 8):
            values = in_ref[peer, start : start + 8, :]
            if start == tile:
                values = jnp.where(here & shared, row, values)
            out_ref[peer, start : start + 8, :] = values


def back_kernel(in_ref, table_ref, out_ref, energy_ref, total_ref):
    total = in_ref[0, SHARE_ROW : SHARE_ROW + 1, :]
    for peer in range(1, PEERS):
        total = total + in_ref[peer, SHARE_ROW : SHARE_ROW + 1, :]
    lane = lane_index(1) - SHARE_LANE
    energy_ref[0] = jnp.sum(jnp.where(lane == 0, total, 0.0))
    energy_ref[1] = jnp.sum(jnp.where(lane == 1, total, 0.0))
    total_ref[0] = jnp.sum(jnp.where(lane == 2, total, 0.0)) / (2 * lax.axis_size("lev"))
    parts = []
    for parity in range(2):
        rows = []
        for slab in range(2):
            for r in range(PITCH // 8):
                columns = []
                for v in range(COLUMNS // 128):
                    pieces = []
                    for place in range(v * GROUP, min((v + 1) * GROUP, SIDE)):
                        read = lambda tile: in_ref[parity * SIDE + place, 8 * tile : 8 * tile + 8, :]
                        pieces += pieces_of(read, slab, r, place % GROUP * WIDTH)
                    columns.append(gather_lanes(pieces))
                rows.append(jnp.concatenate(columns, axis=1))
        high, low = halves(jnp.concatenate(rows, axis=0))
        main = dot(jnp.concatenate([high, low], axis=0), table_ref[parity, 0])
        parts.append(main[:PAIR] + main[PAIR:] + dot(high, table_ref[parity, 1]))
    lower, upper = parts[0] + parts[1], parts[0] - parts[1]
    for slab in range(2):
        rows = slice(slab * PITCH, slab * PITCH + ROWS)
        out_ref[:, slab, :HALF] = lower[rows]
        out_ref[:, slab, HALF:] = upper[rows]


def grant(mebibytes):
    return pltpu.CompilerParams(vmem_limit_bytes=mebibytes << 20)


def in_hbm(array):
    return pltpu.with_memory_space_constraint(array, pltpu.HBM)


VMEM = pl.BlockSpec(memory_space=pltpu.VMEM)
HBM = pl.BlockSpec(memory_space=pltpu.HBM)
SMEM = pl.BlockSpec(memory_space=pltpu.SMEM)


def local(grid_field, truncation_limit, diffusion_order, diffusion_strength, mass_weight):
    row_forward, row_back = row_tables()
    column_forward, column_back = column_tables()
    block = jax.ShapeDtypeStruct((PEERS, 24, 128), jnp.float32)
    levels = lax.axis_size("lev")
    row_steps = 2 * COLUMNS // 256
    sent, lanes, damp = pl.pallas_call(
        row_kernel,
        out_shape=(
            block,
            jax.ShapeDtypeStruct((8, 128), jnp.float32),
            jax.ShapeDtypeStruct((4, QUARTER, 128), jnp.float32),
        ),
        in_specs=[HBM] * 6,
        out_specs=(VMEM, VMEM, VMEM),
        scratch_shapes=[
            pltpu.SMEM((N,), jnp.int32),
            pltpu.SMEM((2,), jnp.int32),
            pltpu.SMEM((2,), jnp.float32),
            pltpu.SMEM((2,), jnp.float32),
            pltpu.VMEM((ROWS, 2, N), jnp.float32),
            pltpu.VMEM((PAIR, 1280), jnp.float32),
            pltpu.VMEM((2, 2 * PAIR, HALF), jnp.bfloat16),
            pltpu.VMEM((row_steps, 2, HALF, 256), jnp.bfloat16),
            pltpu.SemaphoreType.DMA((row_steps + 1,)),
            pltpu.SemaphoreType.DMA((4,)),
        ],
        compiler_params=grant(14),
        name="row_forward",
    )(
        in_hbm(grid_field.transpose(1, 0, 2)),
        in_hbm(jnp.asarray(row_forward)),
        in_hbm(truncation_limit),
        in_hbm(diffusion_order),
        in_hbm(diffusion_strength),
        in_hbm(mass_weight),
    )
    received = lax.all_to_all(sent, "wav", split_axis=0, concat_axis=0, tiled=True)
    damped, share, kept = pl.pallas_call(
        column_kernel,
        out_shape=(
            jax.ShapeDtypeStruct((4, QUARTER, 128), jnp.float32),
            jax.ShapeDtypeStruct((levels, 128), jnp.float32),
            jax.ShapeDtypeStruct((8, 128), jnp.float32),
        ),
        in_specs=[VMEM] * 4,
        out_specs=(VMEM, VMEM, VMEM),
        compiler_params=grant(10),
        name="column_forward",
    )(received, damp, lanes, jnp.asarray(column_forward))
    everyone = lax.all_to_all(share, "lev", split_axis=0, concat_axis=0, tiled=True)
    column_back_call = pl.pallas_call(
        column_back_kernel,
        out_shape=block,
        in_specs=[VMEM, VMEM, HBM],
        out_specs=VMEM,
        scratch_shapes=[
            pltpu.VMEM(column_back.shape, jnp.bfloat16),
            pltpu.VMEM((4, BLOCK, 128), jnp.float32),
            pltpu.SemaphoreType.DMA((4,)),
        ],
        compiler_params=grant(10),
        cost_estimate=pl.CostEstimate(flops=2_000_000_000, bytes_accessed=6_000_000, transcendentals=0),
        name="column_back",
    )
    back = column_back_call(damped, lanes, in_hbm(jnp.asarray(column_back)))
    back = pl.pallas_call(
        share_kernel,
        out_shape=block,
        in_specs=[VMEM] * 3,
        out_specs=VMEM,
        compiler_params=grant(2),
        cost_estimate=pl.CostEstimate(flops=4_000_000_000, bytes_accessed=800_000, transcendentals=0),
        name="share",
    )(back, kept, everyone)
    returned = lax.all_to_all(back, "wav", split_axis=0, concat_axis=0, tiled=True)
    filtered, energies, total_energy = pl.pallas_call(
        back_kernel,
        out_shape=(
            jax.ShapeDtypeStruct((ROWS, 2, N), jnp.float32),
            jax.ShapeDtypeStruct((2,), jnp.float32),
            jax.ShapeDtypeStruct((1,), jnp.float32),
        ),
        in_specs=[VMEM, VMEM],
        out_specs=(VMEM, SMEM, SMEM),
        compiler_params=grant(10),
        name="row_back",
    )(returned, jnp.asarray(row_back))
    return filtered.transpose(1, 0, 2), energies, total_energy.reshape(())


def solution(mesh):
    placed = (P("lev", "wav", None), P(), P("lev"), P("lev"), P("lev"))
    return jax.shard_map(
        local,
        mesh=mesh,
        in_specs=placed,
        out_specs=(P("lev", "wav", None), P("lev"), P()),
        check_vma=False,
    )
```

```python
import functools
import math

import jax
import jax.numpy as jnp
import ml_dtypes
import numpy as np
from jax import lax
from jax.experimental import pallas as pl
from jax.experimental.pallas import tpu as pltpu
from jax.sharding import PartitionSpec as P

N = 1216
HALF = N // 2
QUARTER = N // 4
PEERS = 32
ROWS = N // PEERS
PITCH = 40
WAVES = HALF // PEERS
WIDTH = 2 * WAVES
SIDE = PEERS // 2
GROUP = 3
COLUMNS = -(-SIDE // GROUP) * 128
EVEN_COLUMNS = -(-SIDE // 2 // GROUP) * 128
BLOCK = PEERS // 4 * PITCH
PAIR = 2 * PITCH
SLOTS = {
    (0, 0): [(0, 0, 0, WIDTH)],
    (0, 1): [(1, 0, 0, WIDTH)],
    (0, 2): [(2, 0, 0, WIDTH)],
    (1, 0): [(0, 38, 0, WIDTH)],
    (1, 1): [(1, 38, 0, WIDTH)],
    (1, 2): [(2, 38, 0, WIDTH)],
    (0, 3): [(0, 76, 0, WIDTH)],
    (1, 3): [(1, 76, 0, WIDTH)],
    (0, 4): [(2, 76, 0, WIDTH)],
    (1, 4): [(0, 114, 0, 14), (1, 114, 14, 14), (2, 114, 28, 10)],
}

SHARE_ROW, SHARE_LANE = 16 + ROWS - 32, 76


def split(table):
    high = table.astype(ml_dtypes.bfloat16)
    low = (table - high.astype(np.float64)).astype(ml_dtypes.bfloat16)
    return high, low


def angle(product):
    return (product % N).astype(np.float64) * (2.0 * math.pi / N)


def waves_of(place):
    if place < SIDE:
        return 4, place % (SIDE // 2) * WAVES, place // (SIDE // 2) * 2
    return 2, (place - SIDE) * WAVES, 1


def column_of(place):
    return place // GROUP * 128 + place % GROUP * WIDTH


@functools.cache
def row_tables():
    j = np.arange(HALF)
    even = np.zeros((2, QUARTER, EVEN_COLUMNS))
    odd = np.zeros((HALF, COLUMNS))
    back = np.zeros((2, COLUMNS, HALF))
    for place in range(PEERS):
        stride, first, offset = waves_of(place)
        wave = stride * (first + np.arange(WAVES)) + offset
        theta = angle(j[:, None] * wave[None, :])
        cosine, sine = np.cos(theta), -np.sin(theta)
        weight = np.where(wave == 0, 1.0, 2.0)
        if place == 0:
            sine[:, 0] = np.cos(angle(j * HALF))
        both = np.concatenate([cosine, sine], axis=1)
        start = column_of(place % SIDE)
        back[place // SIDE, start : start + WIDTH, :] = (
            both * np.concatenate([weight, weight]) / float(N) ** 2
        ).T
        if place < SIDE:
            start = column_of(place % (SIDE // 2))
            even[place // (SIDE // 2), :, start : start + WIDTH] = both[:QUARTER]
        else:
            odd[:, start : start + WIDTH] = both
    return np.stack(split(even)), np.stack(split(odd)), np.stack([np.stack(split(t)) for t in back])


@functools.cache
def column_tables():
    place = np.full((PEERS // 4, PITCH), -1, np.int64)
    place[:, :ROWS] = np.arange(QUARTER).reshape(PEERS // 4, ROWS)
    place = place.reshape(-1)
    used = (place >= 0).astype(np.float64)
    spot = np.maximum(place, 0)
    m = np.arange(QUARTER)
    forward, back = [], []
    for residue in range(4):
        theta = angle((4 * m + residue)[:, None] * spot[None, :])
        cosine, sine = np.cos(theta) * used, np.sin(theta) * used
        forward.append(np.concatenate(split(np.concatenate([cosine, sine], axis=1)), axis=0))
        back.append(np.concatenate(split(np.concatenate([cosine.T, -sine.T], axis=1)), axis=0))
    return np.stack(forward), np.stack(back)


def dot(left, right):
    return lax.dot_general(left, right, (((1,), (0,)), ((), ())), preferred_element_type=jnp.float32)


def halves(values):
    high = values.astype(jnp.bfloat16)
    low = (values - high.astype(jnp.float32)).astype(jnp.bfloat16)
    return high, low


def lane_index(rows):
    return lax.broadcasted_iota(jnp.int32, (rows, 128), 1)


def turn(values, shift):
    return values if shift % 128 == 0 else pltpu.roll(values, shift % 128, 1)


def gather_lanes(pieces):
    lane = lane_index(8)
    result = None
    for values, source, target in pieces:
        turned = turn(values, target - source)
        result = turned if result is None else jnp.where(lane >= target, turned, result)
    return result


def packed(read):
    tiles = []
    for tile in range(3):
        pieces = []
        for (slab, r), slots in SLOTS.items():
            for where, lane, first, _ in slots:
                if where == tile:
                    values, start = read(slab, r)
                    pieces.append((values, start + first, lane))
        tiles.append(gather_lanes(sorted(pieces, key=lambda p: p[2])))
    return tiles


def pieces_of(read, slab, r, target):
    return [(read(tile), lane, target + first) for tile, lane, first, _ in SLOTS[slab, r]]


def row_kernel(
    grid_ref, even_in, odd_in, limit_in, order_in, strength_in, mass_in, out_ref, lane_ref, damp_ref,
    limit_ref, order_ref, strength_ref, mass_ref, x_ref, xs, even_ref, odd_ref, sem,
):
    copies = [
        pltpu.make_async_copy(source, target, sem.at[k])
        for k, (source, target) in enumerate(
            [
                (limit_in, limit_ref),
                (order_in, order_ref),
                (strength_in, strength_ref),
                (mass_in, mass_ref),
                (grid_ref, x_ref),
                (even_in, even_ref),
                (odd_in, odd_ref),
            ]
        )
    ]
    for copy in copies:
        copy.start()
    lane_ref[...] = jnp.zeros_like(lane_ref)
    for copy in copies[:4]:
        copy.wait()
    fill_lanes(lane_ref, limit_ref, order_ref, strength_ref, mass_ref)
    fill_damping(lane_ref, damp_ref)
    xs[...] = jnp.zeros_like(xs)
    copies[4].wait()
    for slab in range(2):
        xs[slab * PITCH : slab * PITCH + ROWS, :N] = x_ref[:, slab, :]
    full = xs[...]
    width = full.shape[1]
    shifted = pltpu.roll(full, width - HALF, 1)
    added = full + shifted
    added_shifted = pltpu.roll(added, width - QUARTER, 1)
    values = [
        halves((added + added_shifted)[:, :QUARTER]),
        halves((added - added_shifted)[:, :QUARTER]),
        halves((full - shifted)[:, :HALF]),
    ]
    copies[5].wait()
    copies[6].wait()
    first_place = 0
    for group, (high, low) in enumerate(values):
        table = (lambda part: even_ref[part, group]) if group < 2 else (lambda part: odd_ref[part])
        main = dot(jnp.concatenate([high, low], axis=0), table(0))
        result = main[:PAIR] + main[PAIR:] + dot(high, table(1))
        count = SIDE // 2 if group < 2 else SIDE
        for place in range(count):
            column = column_of(place) // 128 * 128

            def read(slab, r):
                rows = slice(slab * PITCH + 8 * r, slab * PITCH + 8 * r + 8)
                return result[rows, column : column + 128], place % GROUP * WIDTH

            for tile, block in enumerate(packed(read)):
                out_ref[first_place + place, 8 * tile : 8 * tile + 8, :] = block
        first_place += count


def fill_lanes(lane_ref, limit_ref, order_ref, strength_ref, mass_ref):
    place = lax.axis_index("wav")
    stride = jnp.where(place < SIDE, 4, 2)
    first_wave = jnp.where(place < SIDE, place % (SIDE // 2), place - SIDE) * WAVES
    offset = jnp.where(place < SIDE, place // (SIDE // 2) * 2, 1)
    lane = lane_index(1)
    column = lane % 64
    slot = jnp.where(column < WAVES, column, column - WAVES)
    regular = column < WIDTH
    wave = jnp.where(regular, stride * (first_wave + slot) + offset, HALF)
    limit = jnp.broadcast_to(limit_ref[HALF], (1, 128))
    for k in range(WAVES):
        limit = jnp.where(regular & (slot == k), limit_ref[stride * (first_wave + k) + offset], limit)
    weight = jnp.where((wave == 0) | (wave == HALF), 1.0, 2.0) / float(N) ** 4
    top = ((column == WIDTH) | (column == WIDTH + WAVES)) & (place == 0)
    first = lane < 64
    wave = wave.astype(jnp.float32)
    rows = [
        wave * wave,
        limit.astype(jnp.float32),
        jnp.where(first, order_ref[0], order_ref[1]).astype(jnp.float32),
        jnp.where(first, strength_ref[0], strength_ref[1]),
        jnp.where(regular | top, weight, 0.0),
        jnp.where(jnp.broadcast_to(place, (1, 128)) == 0, 1.0, 0.0),
        jnp.where(first, mass_ref[0], mass_ref[1]),
    ]
    for k, row in enumerate(rows):
        lane_ref[k : k + 1, :] = row


def fill_damping(lane_ref, damp_ref):
    wave_square = lane_ref[0:1, :]
    limit = lane_ref[1:2, :]
    order = lane_ref[2:3, :]
    strength = lane_ref[3:4, :]

    @pl.loop(0, 4)
    def _(residue):
        q = 4 * lax.broadcasted_iota(jnp.int32, (QUARTER, 128), 0) + residue
        wave = jnp.where(q < HALF, q, q - N).astype(jnp.float32)
        radius = (wave_square + wave * wave) / (0.5 * N) ** 2
        square = radius * radius
        powered = jnp.where(
            order == 1.0,
            radius,
            jnp.where(order == 2.0, square, jnp.where(order == 3.0, square * radius, square * square)),
        )
        damp_ref[residue] = jnp.where(jnp.abs(wave) <= limit, 1.0 / (1.0 + strength * powered), 0.0)


def turned(values):
    forward = pltpu.roll(values, 128 - WAVES, 1)
    backward = pltpu.roll(values, WAVES, 1)
    spot = lane_index(values.shape[0]) % 64
    return jnp.where((spot < WAVES) | (spot == WIDTH), forward, -backward)


def folded(result):
    count = result.shape[0] // 2
    both = result[:count] + result[count:]
    return both[:, :128] + both[:, 128:]


def weights(values, other):
    return jnp.concatenate(
        [jnp.concatenate(halves(values), axis=1), jnp.concatenate(halves(other), axis=1)], axis=0
    )


def column_kernel(in_ref, damp_ref, lane_ref, table_ref, out_ref, share_ref, kept_ref):
    packs_top = lane_ref[5:6, :] > 0.5
    spot = lane_index(8) % 64
    to_top = (spot == WIDTH) & packs_top
    cleared = ((spot == WAVES) | (spot == WIDTH + WAVES)) & packs_top
    quarters = []
    for quarter in range(4):
        tiles = []
        for peer in range(quarter * PEERS // 4, (quarter + 1) * PEERS // 4):
            read = lambda tile: in_ref[peer, 8 * tile : 8 * tile + 8, :]
            for r in range(PITCH // 8):
                tile = gather_lanes(pieces_of(read, 0, r, 0) + pieces_of(read, 1, r, 64))
                tile = jnp.where(to_top, pltpu.roll(tile, WAVES, 1), jnp.where(cleared, 0.0, tile))
                tiles.append(tile)
        quarters.append(jnp.concatenate(tiles, axis=0))
    c, d = quarters[0] + quarters[2], quarters[1] + quarters[3]
    a, b = quarters[0] - quarters[2], quarters[1] - quarters[3]
    turned_c, turned_d, turned_a, turned_b = turned(c), turned(d), turned(a), turned(b)
    inputs = [
        (c + d, turned_c + turned_d),
        (a + turned_b, turned_a - b),
        (c - d, turned_c - turned_d),
        (a - turned_b, turned_a + b),
    ]
    energy = jnp.zeros((8, 128), jnp.float32)
    for residue in range(4):
        damped = folded(dot(table_ref[residue], weights(*inputs[residue]))) * damp_ref[residue]
        out_ref[residue] = damped
        energy = energy + jnp.sum((damped * damped).reshape(QUARTER // 8, 8, 128), axis=0)
    energy = jnp.sum(energy, axis=0, keepdims=True) * lane_ref[4:5, :]
    lane = lane_index(1)
    first = jnp.sum(jnp.where(lane < 64, energy, 0.0), axis=1, keepdims=True)
    second = jnp.sum(jnp.where(lane < 64, 0.0, energy), axis=1, keepdims=True)
    weighted = jnp.sum(energy * lane_ref[6:7, :], axis=1, keepdims=True)
    row = jnp.where(lane == 0, first, jnp.where(lane == 1, second, jnp.where(lane == 2, weighted, 0.0)))
    share_ref[...] = jnp.broadcast_to(row, share_ref.shape)
    kept_ref[...] = jnp.broadcast_to(row, kept_ref.shape)


def column_back_kernel(in_ref, lane_ref, table_ref, out_ref, held, parts, sem):
    def table_copy(residue):
        return pltpu.make_async_copy(table_ref.at[residue], held.at[residue], sem.at[residue])

    for residue in range(4):
        table_copy(residue).start()
    packs_top = lane_ref[5:6, :] > 0.5
    peers = 2
    rows = peers * PITCH

    @pl.loop(0, 4)
    def _(residue):
        damped = in_ref[residue]
        table_copy(residue).wait()
        parts[residue] = folded(dot(held[residue], weights(damped, turned(damped))))

    @pl.loop(0, PEERS // 4 // peers)
    def _(step):
        start = pl.multiple_of(step * rows, rows)
        part = [parts[residue, pl.ds(start, rows), :] for residue in range(4)]
        even, odd = part[0] + part[2], part[1] + part[3]
        even_less, odd_less = part[0] - part[2], turned(part[1] - part[3])
        from_top = (lane_index(8) % 64 == WAVES) & packs_top
        for quarter, grid in enumerate([even + odd, even_less - odd_less, even - odd, even_less + odd_less]):
            for k in range(peers):
                fixed = {}
                for r in range(PITCH // 8):
                    tile = grid[k * PITCH + 8 * r : k * PITCH + 8 * r + 8]
                    fixed[r] = jnp.where(from_top, pltpu.roll(tile, 128 - WAVES, 1), tile)
                for tile, values in enumerate(packed(lambda slab, r: (fixed[r], 64 * slab))):
                    out_ref[quarter * (PEERS // 4) + step * peers + k, 8 * tile : 8 * tile + 8, :] = values


def share_kernel(in_ref, share_ref, everyone_ref, out_ref):
    lane = lane_index(1)
    levels = jnp.sum(everyone_ref[...], axis=0, keepdims=True)
    row = pltpu.roll(jnp.where(lane == 2, levels, share_ref[0:1, :]), SHARE_LANE, 1)
    shared = (lane >= SHARE_LANE) & (lane < SHARE_LANE + 3)
    tile = SHARE_ROW // 8 * 8
    here = lax.broadcasted_iota(jnp.int32, (8, 128), 0) == SHARE_ROW - tile
    for peer in range(PEERS):
        for start in range(0, 24, 8):
            values = in_ref[peer, start : start + 8, :]
            if start == tile:
                values = jnp.where(here & shared, row, values)
            out_ref[peer, start : start + 8, :] = values


def back_kernel(in_ref, table_ref, out_ref, energy_ref, total_ref):
    total = in_ref[0, SHARE_ROW : SHARE_ROW + 1, :]
    for peer in range(1, PEERS):
        total = total + in_ref[peer, SHARE_ROW : SHARE_ROW + 1, :]
    lane = lane_index(1) - SHARE_LANE
    energy_ref[0] = jnp.sum(jnp.where(lane == 0, total, 0.0))
    energy_ref[1] = jnp.sum(jnp.where(lane == 1, total, 0.0))
    total_ref[0] = jnp.sum(jnp.where(lane == 2, total, 0.0)) / (2 * lax.axis_size("lev"))
    parts = []
    for parity in range(2):
        rows = []
        for slab in range(2):
            for r in range(PITCH // 8):
                columns = []
                for v in range(COLUMNS // 128):
                    pieces = []
                    for place in range(v * GROUP, min((v + 1) * GROUP, SIDE)):
                        read = lambda tile: in_ref[parity * SIDE + place, 8 * tile : 8 * tile + 8, :]
                        pieces += pieces_of(read, slab, r, place % GROUP * WIDTH)
                    columns.append(gather_lanes(pieces))
                rows.append(jnp.concatenate(columns, axis=1))
        high, low = halves(jnp.concatenate(rows, axis=0))
        main = dot(jnp.concatenate([high, low], axis=0), table_ref[parity, 0])
        parts.append(main[:PAIR] + main[PAIR:] + dot(high, table_ref[parity, 1]))
    lower, upper = parts[0] + parts[1], parts[0] - parts[1]
    for slab in range(2):
        rows = slice(slab * PITCH, slab * PITCH + ROWS)
        out_ref[:, slab, :HALF] = lower[rows]
        out_ref[:, slab, HALF:] = upper[rows]


def grant(mebibytes):
    return pltpu.CompilerParams(vmem_limit_bytes=mebibytes << 20)


def in_hbm(array):
    return pltpu.with_memory_space_constraint(array, pltpu.HBM)


VMEM = pl.BlockSpec(memory_space=pltpu.VMEM)
HBM = pl.BlockSpec(memory_space=pltpu.HBM)
SMEM = pl.BlockSpec(memory_space=pltpu.SMEM)


def local(grid_field, truncation_limit, diffusion_order, diffusion_strength, mass_weight):
    row_even, row_odd, row_back = row_tables()
    column_forward, column_back = column_tables()
    block = jax.ShapeDtypeStruct((PEERS, 24, 128), jnp.float32)
    levels = lax.axis_size("lev")
    sent, lanes, damp = pl.pallas_call(
        row_kernel,
        out_shape=(
            block,
            jax.ShapeDtypeStruct((8, 128), jnp.float32),
            jax.ShapeDtypeStruct((4, QUARTER, 128), jnp.float32),
        ),
        in_specs=[HBM] * 7,
        out_specs=(VMEM, VMEM, VMEM),
        scratch_shapes=[
            pltpu.SMEM((N,), jnp.int32),
            pltpu.SMEM((2,), jnp.int32),
            pltpu.SMEM((2,), jnp.float32),
            pltpu.SMEM((2,), jnp.float32),
            pltpu.VMEM((ROWS, 2, N), jnp.float32),
            pltpu.VMEM((PAIR, 1280), jnp.float32),
            pltpu.VMEM(row_even.shape, jnp.bfloat16),
            pltpu.VMEM(row_odd.shape, jnp.bfloat16),
            pltpu.SemaphoreType.DMA((7,)),
        ],
        compiler_params=grant(14),
        name="row_forward",
    )(
        in_hbm(grid_field.transpose(1, 0, 2)),
        in_hbm(jnp.asarray(row_even)),
        in_hbm(jnp.asarray(row_odd)),
        in_hbm(truncation_limit),
        in_hbm(diffusion_order),
        in_hbm(diffusion_strength),
        in_hbm(mass_weight),
    )
    received = lax.all_to_all(sent, "wav", split_axis=0, concat_axis=0, tiled=True)
    damped, share, kept = pl.pallas_call(
        column_kernel,
        out_shape=(
            jax.ShapeDtypeStruct((4, QUARTER, 128), jnp.float32),
            jax.ShapeDtypeStruct((levels, 128), jnp.float32),
            jax.ShapeDtypeStruct((8, 128), jnp.float32),
        ),
        in_specs=[VMEM] * 4,
        out_specs=(VMEM, VMEM, VMEM),
        compiler_params=grant(10),
        name="column_forward",
    )(received, damp, lanes, jnp.asarray(column_forward))
    everyone = lax.all_to_all(share, "lev", split_axis=0, concat_axis=0, tiled=True)
    column_back_call = pl.pallas_call(
        column_back_kernel,
        out_shape=block,
        in_specs=[VMEM, VMEM, HBM],
        out_specs=VMEM,
        scratch_shapes=[
            pltpu.VMEM(column_back.shape, jnp.bfloat16),
            pltpu.VMEM((4, BLOCK, 128), jnp.float32),
            pltpu.SemaphoreType.DMA((4,)),
        ],
        compiler_params=grant(10),
        cost_estimate=pl.CostEstimate(flops=2_000_000_000, bytes_accessed=6_000_000, transcendentals=0),
        name="column_back",
    )
    back = column_back_call(damped, lanes, in_hbm(jnp.asarray(column_back)))
    back = pl.pallas_call(
        share_kernel,
        out_shape=block,
        in_specs=[VMEM] * 3,
        out_specs=VMEM,
        compiler_params=grant(2),
        cost_estimate=pl.CostEstimate(flops=4_000_000_000, bytes_accessed=800_000, transcendentals=0),
        name="share",
    )(back, kept, everyone)
    returned = lax.all_to_all(back, "wav", split_axis=0, concat_axis=0, tiled=True)
    filtered, energies, total_energy = pl.pallas_call(
        back_kernel,
        out_shape=(
            jax.ShapeDtypeStruct((ROWS, 2, N), jnp.float32),
            jax.ShapeDtypeStruct((2,), jnp.float32),
            jax.ShapeDtypeStruct((1,), jnp.float32),
        ),
        in_specs=[VMEM, VMEM],
        out_specs=(VMEM, SMEM, SMEM),
        compiler_params=grant(10),
        name="row_back",
    )(returned, jnp.asarray(row_back))
    return filtered.transpose(1, 0, 2), energies, total_energy.reshape(())


def solution(mesh):
    placed = (P("lev", "wav", None), P(), P("lev"), P("lev"), P("lev"))
    return jax.shard_map(
        local,
        mesh=mesh,
        in_specs=placed,
        out_specs=(P("lev", "wav", None), P("lev"), P()),
        check_vma=False,
    )
```

```python
import functools
import math

import jax
import jax.numpy as jnp
import ml_dtypes
import numpy as np
from jax import lax
from jax.experimental import pallas as pl
from jax.experimental.pallas import tpu as pltpu
from jax.sharding import PartitionSpec as P

N = 1216
HALF = N // 2
QUARTER = N // 4
EIGHTH = N // 8
PEERS = 32
ROWS = N // PEERS
PITCH = 40
WAVES = HALF // PEERS
WIDTH = 2 * WAVES
SIDE = PEERS // 2
GROUP = 3
COLUMNS = -(-SIDE // GROUP) * 128
EVEN_COLUMNS = -(-SIDE // 2 // GROUP) * 128
BLOCK = PEERS // 4 * PITCH
PAIR = 2 * PITCH
SLOTS = {
    (0, 0): [(0, 0, 0, WIDTH)],
    (0, 1): [(1, 0, 0, WIDTH)],
    (0, 2): [(2, 0, 0, WIDTH)],
    (1, 0): [(0, 38, 0, WIDTH)],
    (1, 1): [(1, 38, 0, WIDTH)],
    (1, 2): [(2, 38, 0, WIDTH)],
    (0, 3): [(0, 76, 0, WIDTH)],
    (1, 3): [(1, 76, 0, WIDTH)],
    (0, 4): [(2, 76, 0, WIDTH)],
    (1, 4): [(0, 114, 0, 14), (1, 114, 14, 14), (2, 114, 28, 10)],
}

SHARE_ROW, SHARE_LANE = 16 + ROWS - 32, 76


def split(table):
    high = table.astype(ml_dtypes.bfloat16)
    low = (table - high.astype(np.float64)).astype(ml_dtypes.bfloat16)
    return high, low


def angle(product):
    return (product % N).astype(np.float64) * (2.0 * math.pi / N)


def waves_of(place):
    if place < SIDE:
        return 4, place % (SIDE // 2) * WAVES, place // (SIDE // 2) * 2
    return 2, (place - SIDE) * WAVES, 1


def column_of(place):
    return place // GROUP * 128 + place % GROUP * WIDTH


@functools.cache
def row_tables():
    j = np.arange(HALF)
    even = np.zeros((2, QUARTER, EVEN_COLUMNS))
    odd = np.zeros((HALF, COLUMNS))
    back = np.zeros((2, COLUMNS, HALF))
    for place in range(PEERS):
        stride, first, offset = waves_of(place)
        wave = stride * (first + np.arange(WAVES)) + offset
        theta = angle(j[:, None] * wave[None, :])
        cosine, sine = np.cos(theta), -np.sin(theta)
        weight = np.where(wave == 0, 1.0, 2.0)
        if place == 0:
            sine[:, 0] = np.cos(angle(j * HALF))
        both = np.concatenate([cosine, sine], axis=1)
        start = column_of(place % SIDE)
        back[place // SIDE, start : start + WIDTH, :] = (
            both * np.concatenate([weight, weight]) / float(N) ** 2
        ).T
        if place < SIDE:
            start = column_of(place % (SIDE // 2))
            even[place // (SIDE // 2), :, start : start + WIDTH] = both[:QUARTER]
        else:
            odd[:, start : start + WIDTH] = both
    return np.stack(split(even)), np.stack(split(odd)), np.stack([np.stack(split(t)) for t in back])


def padded_rows(peers):
    place = np.full((peers, PITCH), -1, np.int64)
    place[:, :ROWS] = np.arange(peers * ROWS).reshape(peers, ROWS)
    place = place.reshape(-1)
    return np.maximum(place, 0), (place >= 0).astype(np.float64)


@functools.cache
def column_tables():
    m = np.arange(EIGHTH)
    forward, back = [], []
    spot, used = padded_rows(PEERS // 8)
    for residue in range(8):
        theta = angle((8 * m + residue)[:, None] * spot[None, :])
        cosine, sine = np.cos(theta) * used, np.sin(theta) * used
        forward.append(np.concatenate(split(np.concatenate([cosine, sine], axis=1)), axis=0))
    spot, used = padded_rows(PEERS // 4)
    for residue in range(4):
        q = np.concatenate([8 * m + residue, 8 * m + residue + 4])
        theta = angle(spot[:, None] * q[None, :])
        cosine, sine = np.cos(theta) * used[:, None], np.sin(theta) * used[:, None]
        back.append(np.concatenate(split(np.concatenate([cosine, -sine], axis=1)), axis=0))
    return np.stack(forward), np.stack(back)


def dot(left, right):
    return lax.dot_general(left, right, (((1,), (0,)), ((), ())), preferred_element_type=jnp.float32)


def halves(values):
    high = values.astype(jnp.bfloat16)
    low = (values - high.astype(jnp.float32)).astype(jnp.bfloat16)
    return high, low


def lane_index(rows):
    return lax.broadcasted_iota(jnp.int32, (rows, 128), 1)


def turn(values, shift):
    return values if shift % 128 == 0 else pltpu.roll(values, shift % 128, 1)


def gather_lanes(pieces):
    lane = lane_index(8)
    result = None
    for values, source, target in pieces:
        turned = turn(values, target - source)
        result = turned if result is None else jnp.where(lane >= target, turned, result)
    return result


def packed(read):
    tiles = []
    for tile in range(3):
        pieces = []
        for (slab, r), slots in SLOTS.items():
            for where, lane, first, _ in slots:
                if where == tile:
                    values, start = read(slab, r)
                    pieces.append((values, start + first, lane))
        tiles.append(gather_lanes(sorted(pieces, key=lambda p: p[2])))
    return tiles


def pieces_of(read, slab, r, target):
    return [(read(tile), lane, target + first) for tile, lane, first, _ in SLOTS[slab, r]]


def row_kernel(
    grid_ref, even_in, odd_in, limit_in, order_in, strength_in, mass_in, out_ref, lane_ref, damp_ref,
    limit_ref, order_ref, strength_ref, mass_ref, x_ref, xs, even_ref, odd_ref, sem,
):
    copies = [
        pltpu.make_async_copy(source, target, sem.at[k])
        for k, (source, target) in enumerate(
            [
                (limit_in, limit_ref),
                (order_in, order_ref),
                (strength_in, strength_ref),
                (mass_in, mass_ref),
                (grid_ref, x_ref),
                (even_in, even_ref),
                (odd_in, odd_ref),
            ]
        )
    ]
    for copy in copies:
        copy.start()
    lane_ref[...] = jnp.zeros_like(lane_ref)
    for copy in copies[:4]:
        copy.wait()
    fill_lanes(lane_ref, limit_ref, order_ref, strength_ref, mass_ref)
    fill_damping(lane_ref, damp_ref)
    xs[...] = jnp.zeros_like(xs)
    copies[4].wait()
    for slab in range(2):
        xs[slab * PITCH : slab * PITCH + ROWS, :N] = x_ref[:, slab, :]
    full = xs[...]
    width = full.shape[1]
    shifted = pltpu.roll(full, width - HALF, 1)
    added = full + shifted
    added_shifted = pltpu.roll(added, width - QUARTER, 1)
    values = [
        halves((added + added_shifted)[:, :QUARTER]),
        halves((added - added_shifted)[:, :QUARTER]),
        halves((full - shifted)[:, :HALF]),
    ]
    copies[5].wait()
    copies[6].wait()
    first_place = 0
    for group, (high, low) in enumerate(values):
        table = (lambda part: even_ref[part, group]) if group < 2 else (lambda part: odd_ref[part])
        main = dot(jnp.concatenate([high, low], axis=0), table(0))
        result = main[:PAIR] + main[PAIR:] + dot(high, table(1))
        count = SIDE // 2 if group < 2 else SIDE
        for place in range(count):
            column = column_of(place) // 128 * 128

            def read(slab, r):
                rows = slice(slab * PITCH + 8 * r, slab * PITCH + 8 * r + 8)
                return result[rows, column : column + 128], place % GROUP * WIDTH

            for tile, block in enumerate(packed(read)):
                out_ref[first_place + place, 8 * tile : 8 * tile + 8, :] = block
        first_place += count


def fill_lanes(lane_ref, limit_ref, order_ref, strength_ref, mass_ref):
    place = lax.axis_index("wav")
    stride = jnp.where(place < SIDE, 4, 2)
    first_wave = jnp.where(place < SIDE, place % (SIDE // 2), place - SIDE) * WAVES
    offset = jnp.where(place < SIDE, place // (SIDE // 2) * 2, 1)
    lane = lane_index(1)
    column = lane % 64
    slot = jnp.where(column < WAVES, column, column - WAVES)
    regular = column < WIDTH
    wave = jnp.where(regular, stride * (first_wave + slot) + offset, HALF)
    limit = jnp.broadcast_to(limit_ref[HALF], (1, 128))
    for k in range(WAVES):
        limit = jnp.where(regular & (slot == k), limit_ref[stride * (first_wave + k) + offset], limit)
    weight = jnp.where((wave == 0) | (wave == HALF), 1.0, 2.0) / float(N) ** 4
    top = ((column == WIDTH) | (column == WIDTH + WAVES)) & (place == 0)
    first = lane < 64
    wave = wave.astype(jnp.float32)
    rows = [
        wave * wave,
        limit.astype(jnp.float32),
        jnp.where(first, order_ref[0], order_ref[1]).astype(jnp.float32),
        jnp.where(first, strength_ref[0], strength_ref[1]),
        jnp.where(regular | top, weight, 0.0),
        jnp.where(jnp.broadcast_to(place, (1, 128)) == 0, 1.0, 0.0),
        jnp.where(first, mass_ref[0], mass_ref[1]),
    ]
    for k, row in enumerate(rows):
        lane_ref[k : k + 1, :] = row


def fill_damping(lane_ref, damp_ref):
    wave_square = lane_ref[0:1, :]
    limit = lane_ref[1:2, :]
    order = lane_ref[2:3, :]
    strength = lane_ref[3:4, :]

    @pl.loop(0, 4)
    def _(residue):
        row = lax.broadcasted_iota(jnp.int32, (QUARTER, 128), 0)
        q = jnp.where(row < EIGHTH, 8 * row, 8 * (row - EIGHTH) + 4) + residue
        wave = jnp.where(q < HALF, q, q - N).astype(jnp.float32)
        radius = (wave_square + wave * wave) / (0.5 * N) ** 2
        square = radius * radius
        powered = jnp.where(
            order == 1.0,
            radius,
            jnp.where(order == 2.0, square, jnp.where(order == 3.0, square * radius, square * square)),
        )
        damp_ref[residue] = jnp.where(jnp.abs(wave) <= limit, 1.0 / (1.0 + strength * powered), 0.0)


def turned(values):
    forward = pltpu.roll(values, 128 - WAVES, 1)
    backward = pltpu.roll(values, WAVES, 1)
    spot = lane_index(values.shape[0]) % 64
    return jnp.where((spot < WAVES) | (spot == WIDTH), forward, -backward)


def folded(result):
    count = result.shape[0] // 2
    both = result[:count] + result[count:]
    return both[:, :128] + both[:, 128:]


def weights(values, other):
    return jnp.concatenate(
        [jnp.concatenate(halves(values), axis=1), jnp.concatenate(halves(other), axis=1)], axis=0
    )


def column_kernel(in_ref, damp_ref, lane_ref, table_ref, out_ref, share_ref, kept_ref):
    packs_top = lane_ref[5:6, :] > 0.5
    spot = lane_index(8) % 64
    to_top = (spot == WIDTH) & packs_top
    cleared = ((spot == WAVES) | (spot == WIDTH + WAVES)) & packs_top
    eighths = []
    for eighth in range(8):
        tiles = []
        for peer in range(eighth * PEERS // 8, (eighth + 1) * PEERS // 8):
            read = lambda tile: in_ref[peer, 8 * tile : 8 * tile + 8, :]
            for r in range(PITCH // 8):
                tile = gather_lanes(pieces_of(read, 0, r, 0) + pieces_of(read, 1, r, 64))
                tile = jnp.where(to_top, pltpu.roll(tile, WAVES, 1), jnp.where(cleared, 0.0, tile))
                tiles.append(tile)
        eighths.append(jnp.concatenate(tiles, axis=0))
    added = [eighths[k] + eighths[k + 4] for k in range(4)]
    less = [eighths[k] - eighths[k + 4] for k in range(4)]
    less_turned = [turned(v) for v in less]
    root = math.sqrt(0.5)
    odd = [
        (less[0], less_turned[0]),
        (root * (less[1] + less_turned[1]), root * (less_turned[1] - less[1])),
        (less_turned[2], -less[2]),
        (root * (less_turned[3] - less[3]), -root * (less_turned[3] + less[3])),
    ]
    c, d, a, b = added[0] + added[2], added[1] + added[3], added[0] - added[2], added[1] - added[3]
    even_terms = [(v, turned(v)) for v in (c, d, a, b)]
    plus = lambda u, v: (u[0] + v[0], u[1] + v[1])
    minus = lambda u, v: (u[0] - v[0], u[1] - v[1])
    odd_terms = [plus(odd[0], odd[2]), plus(odd[1], odd[3]), minus(odd[0], odd[2]), minus(odd[1], odd[3])]
    inputs = [None] * 8
    for offset, (c, d, a, b) in enumerate((even_terms, odd_terms)):
        b = (b[1], -b[0])
        inputs[offset :: 2] = [plus(c, d), plus(a, b), minus(c, d), minus(a, b)]
    energy = jnp.zeros((8, 128), jnp.float32)
    for residue in range(8):
        rows = slice(residue // 4 * EIGHTH, (residue // 4 + 1) * EIGHTH)
        damped = folded(dot(table_ref[residue], weights(*inputs[residue]))) * damp_ref[residue % 4, rows, :]
        out_ref[residue % 4, rows, :] = damped
        energy = energy + jnp.sum((damped * damped).reshape(EIGHTH // 8, 8, 128), axis=0)
    energy = jnp.sum(energy, axis=0, keepdims=True) * lane_ref[4:5, :]
    lane = lane_index(1)
    first = jnp.sum(jnp.where(lane < 64, energy, 0.0), axis=1, keepdims=True)
    second = jnp.sum(jnp.where(lane < 64, 0.0, energy), axis=1, keepdims=True)
    weighted = jnp.sum(energy * lane_ref[6:7, :], axis=1, keepdims=True)
    row = jnp.where(lane == 0, first, jnp.where(lane == 1, second, jnp.where(lane == 2, weighted, 0.0)))
    share_ref[...] = jnp.broadcast_to(row, share_ref.shape)
    kept_ref[...] = jnp.broadcast_to(row, kept_ref.shape)


def column_back_kernel(in_ref, lane_ref, table_ref, out_ref, held, parts, sem):
    def table_copy(residue):
        return pltpu.make_async_copy(table_ref.at[residue], held.at[residue], sem.at[residue])

    for residue in range(4):
        table_copy(residue).start()
    packs_top = lane_ref[5:6, :] > 0.5
    peers = 2
    rows = peers * PITCH

    @pl.loop(0, 4)
    def _(residue):
        damped = in_ref[residue]
        table_copy(residue).wait()
        parts[residue] = folded(dot(held[residue], weights(damped, turned(damped))))

    @pl.loop(0, PEERS // 4 // peers)
    def _(step):
        start = pl.multiple_of(step * rows, rows)
        part = [parts[residue, pl.ds(start, rows), :] for residue in range(4)]
        even, odd = part[0] + part[2], part[1] + part[3]
        even_less, odd_less = part[0] - part[2], turned(part[1] - part[3])
        from_top = (lane_index(8) % 64 == WAVES) & packs_top
        for quarter, grid in enumerate([even + odd, even_less - odd_less, even - odd, even_less + odd_less]):
            for k in range(peers):
                fixed = {}
                for r in range(PITCH // 8):
                    tile = grid[k * PITCH + 8 * r : k * PITCH + 8 * r + 8]
                    fixed[r] = jnp.where(from_top, pltpu.roll(tile, 128 - WAVES, 1), tile)
                for tile, values in enumerate(packed(lambda slab, r: (fixed[r], 64 * slab))):
                    out_ref[quarter * (PEERS // 4) + step * peers + k, 8 * tile : 8 * tile + 8, :] = values


def share_kernel(in_ref, share_ref, everyone_ref, out_ref):
    lane = lane_index(1)
    levels = jnp.sum(everyone_ref[...], axis=0, keepdims=True)
    row = pltpu.roll(jnp.where(lane == 2, levels, share_ref[0:1, :]), SHARE_LANE, 1)
    shared = (lane >= SHARE_LANE) & (lane < SHARE_LANE + 3)
    tile = SHARE_ROW // 8 * 8
    here = lax.broadcasted_iota(jnp.int32, (8, 128), 0) == SHARE_ROW - tile
    for peer in range(PEERS):
        for start in range(0, 24, 8):
            values = in_ref[peer, start : start + 8, :]
            if start == tile:
                values = jnp.where(here & shared, row, values)
            out_ref[peer, start : start + 8, :] = values


def back_kernel(in_ref, table_ref, out_ref, energy_ref, total_ref):
    parts = []
    for parity in range(2):
        rows = []
        for slab in range(2):
            for r in range(PITCH // 8):
                columns = []
                for v in range(COLUMNS // 128):
                    pieces = []
                    for place in range(v * GROUP, min((v + 1) * GROUP, SIDE)):
                        read = lambda tile: in_ref[parity * SIDE + place, 8 * tile : 8 * tile + 8, :]
                        pieces += pieces_of(read, slab, r, place % GROUP * WIDTH)
                    columns.append(gather_lanes(pieces))
                rows.append(jnp.concatenate(columns, axis=1))
        high, low = halves(jnp.concatenate(rows, axis=0))
        main = dot(jnp.concatenate([high, low], axis=0), table_ref[parity, 0])
        parts.append(main[:PAIR] + main[PAIR:] + dot(high, table_ref[parity, 1]))
    lower, upper = parts[0] + parts[1], parts[0] - parts[1]
    for slab in range(2):
        rows = slice(slab * PITCH, slab * PITCH + ROWS)
        out_ref[:, slab, :HALF] = lower[rows]
        out_ref[:, slab, HALF:] = upper[rows]
    total = in_ref[0, SHARE_ROW : SHARE_ROW + 1, :]
    for peer in range(1, PEERS):
        total = total + in_ref[peer, SHARE_ROW : SHARE_ROW + 1, :]
    lane = lane_index(1) - SHARE_LANE
    energy_ref[0] = jnp.sum(jnp.where(lane == 0, total, 0.0))
    energy_ref[1] = jnp.sum(jnp.where(lane == 1, total, 0.0))
    total_ref[0] = jnp.sum(jnp.where(lane == 2, total, 0.0)) / (2 * lax.axis_size("lev"))


def grant(mebibytes):
    return pltpu.CompilerParams(vmem_limit_bytes=mebibytes << 20)


def in_hbm(array):
    return pltpu.with_memory_space_constraint(array, pltpu.HBM)


VMEM = pl.BlockSpec(memory_space=pltpu.VMEM)
HBM = pl.BlockSpec(memory_space=pltpu.HBM)
SMEM = pl.BlockSpec(memory_space=pltpu.SMEM)


def local(grid_field, truncation_limit, diffusion_order, diffusion_strength, mass_weight):
    row_even, row_odd, row_back = row_tables()
    column_forward, column_back = column_tables()
    block = jax.ShapeDtypeStruct((PEERS, 24, 128), jnp.float32)
    levels = lax.axis_size("lev")
    sent, lanes, damp = pl.pallas_call(
        row_kernel,
        out_shape=(
            block,
            jax.ShapeDtypeStruct((8, 128), jnp.float32),
            jax.ShapeDtypeStruct((4, QUARTER, 128), jnp.float32),
        ),
        in_specs=[HBM] * 7,
        out_specs=(VMEM, VMEM, VMEM),
        scratch_shapes=[
            pltpu.SMEM((N,), jnp.int32),
            pltpu.SMEM((2,), jnp.int32),
            pltpu.SMEM((2,), jnp.float32),
            pltpu.SMEM((2,), jnp.float32),
            pltpu.VMEM((ROWS, 2, N), jnp.float32),
            pltpu.VMEM((PAIR, 1280), jnp.float32),
            pltpu.VMEM(row_even.shape, jnp.bfloat16),
            pltpu.VMEM(row_odd.shape, jnp.bfloat16),
            pltpu.SemaphoreType.DMA((7,)),
        ],
        compiler_params=grant(14),
        name="row_forward",
    )(
        in_hbm(grid_field.transpose(1, 0, 2)),
        in_hbm(jnp.asarray(row_even)),
        in_hbm(jnp.asarray(row_odd)),
        in_hbm(truncation_limit),
        in_hbm(diffusion_order),
        in_hbm(diffusion_strength),
        in_hbm(mass_weight),
    )
    received = lax.all_to_all(sent, "wav", split_axis=0, concat_axis=0, tiled=True)
    damped, share, kept = pl.pallas_call(
        column_kernel,
        out_shape=(
            jax.ShapeDtypeStruct((4, QUARTER, 128), jnp.float32),
            jax.ShapeDtypeStruct((levels, 128), jnp.float32),
            jax.ShapeDtypeStruct((8, 128), jnp.float32),
        ),
        in_specs=[VMEM] * 4,
        out_specs=(VMEM, VMEM, VMEM),
        compiler_params=grant(10),
        name="column_forward",
    )(received, damp, lanes, jnp.asarray(column_forward))
    everyone = lax.all_to_all(share, "lev", split_axis=0, concat_axis=0, tiled=True)
    column_back_call = pl.pallas_call(
        column_back_kernel,
        out_shape=block,
        in_specs=[VMEM, VMEM, HBM],
        out_specs=VMEM,
        scratch_shapes=[
            pltpu.VMEM(column_back.shape, jnp.bfloat16),
            pltpu.VMEM((4, BLOCK, 128), jnp.float32),
            pltpu.SemaphoreType.DMA((4,)),
        ],
        compiler_params=grant(10),
        cost_estimate=pl.CostEstimate(flops=2_000_000_000, bytes_accessed=6_000_000, transcendentals=0),
        name="column_back",
    )
    back = column_back_call(damped, lanes, in_hbm(jnp.asarray(column_back)))
    back = pl.pallas_call(
        share_kernel,
        out_shape=block,
        in_specs=[VMEM] * 3,
        out_specs=VMEM,
        compiler_params=grant(2),
        cost_estimate=pl.CostEstimate(flops=4_000_000_000, bytes_accessed=800_000, transcendentals=0),
        name="share",
    )(back, kept, everyone)
    returned = lax.all_to_all(back, "wav", split_axis=0, concat_axis=0, tiled=True)
    filtered, energies, total_energy = pl.pallas_call(
        back_kernel,
        out_shape=(
            jax.ShapeDtypeStruct((ROWS, 2, N), jnp.float32),
            jax.ShapeDtypeStruct((2,), jnp.float32),
            jax.ShapeDtypeStruct((1,), jnp.float32),
        ),
        in_specs=[VMEM, VMEM],
        out_specs=(VMEM, SMEM, SMEM),
        compiler_params=grant(10),
        name="row_back",
    )(returned, jnp.asarray(row_back))
    return filtered.transpose(1, 0, 2), energies, total_energy.reshape(())


def solution(mesh):
    placed = (P("lev", "wav", None), P(), P("lev"), P("lev"), P("lev"))
    return jax.shard_map(
        local,
        mesh=mesh,
        in_specs=placed,
        out_specs=(P("lev", "wav", None), P("lev"), P()),
        check_vma=False,
    )
```
